256 devices in a mesh: gz: 64 (over z, x, core), gy: 4 (over y).
Axes of the slice: x: 4, y: 4, z: 8, core: 2. Of those that a mesh axis runs over, the one named last changes fastest.
Arguments:
- iterate: float32 [128, 256, 1024], P('gz', 'gy'), may hold values from -1.5 to 1.5
- basis: bfloat16 [32, 128, 256, 1024], P(None, 'gz', 'gy'), may hold values from -6 to 6
- coeffs: float32 [32], replicated, may hold values from -0.3125 to 0.3125
- rhs: float32 [128, 256, 1024], P('gz', 'gy'), may hold values from -8 to 8
- kappa: float32 [128, 256, 1024], P('gz', 'gy'), may hold values from 0.5 to 4
- offsets: int32 [128, 256, 8], P('gz', 'gy'), may hold values from 0 to 2047
- flips: int32 [128, 256, 8], P('gz', 'gy'), may hold values from 0 to 1
Outputs:
- new_iterate: float32 [128, 256, 1024], P('gz', 'gy')
- residual: float32 [128, 256, 1024], P('gz', 'gy')
- sketch_unit: float32 [2048], replicated
The draws below stay inside these ranges and needn't reach their ends.
All inputs are finite; a program needn't handle non-finite values.
Results may differ from the reference program's by a relative error of at most 0.00058.
Values sent between devices are 32-bit elements; how exact they have to be, the bound alone decides.
No kernel may reach another device: no remote copies, remote signals or barrier semaphores. Data moves between devices by JAX's collectives and lax.ppermute only.
A program may use at most 64 MiB of HBM per device.

```python
import math
import jax
import jax.numpy as jnp
from jax import lax

NX = 1024
KB = 32
SK = 2048
BLK = 128
NZ = 128
NY = 256


def plant(array, key, least, high):
    shape = array.shape
    spot = [jax.random.randint(jax.random.fold_in(key, axis), (), 0, shape[axis]) for axis in range(len(shape))]
    array = array.at[tuple(spot)].set(least)
    longest = shape.index(max(shape))
    spot[longest] = (spot[longest] + 1) % shape[longest]
    return array.at[tuple(spot)].set(high)


def block_scale(stream_key, dims, shards, low, high):
    def one(axis_at, shards_of):
        draws = jax.random.uniform(jax.random.fold_in(jax.random.fold_in(stream_key, 6), axis_at), (shards_of,), jnp.float32, low / len(shards), high / len(shards))
        return jnp.repeat(jnp.exp(draws), dims[axis_at] // shards_of).reshape((-1,) + (1,) * (len(dims) - axis_at - 1))

    gain = one(*shards[0])
    for cut in shards[1:]:
        gain = gain * one(*cut)
    return gain


def normal_values(rng, extent, scale, bound, shards=(), kind=jnp.bfloat16):
    loudness = block_scale(rng, extent, shards, -0.22, 0.18) if shards else 1.0
    drawn = jax.random.normal(rng, extent, jnp.float32) * scale * loudness
    return jnp.minimum(jnp.maximum(drawn, -bound), bound).astype(kind)


def setup_inputs(seed: int = 0) -> dict:
    keys = jax.random.split(jax.random.key(seed), 8)
    iterate = normal_values(keys[0], (NZ, NY, NX), 0.1, 1.5, ((0, 64), (1, 4)), jnp.float32)
    basis = normal_values(keys[1], (KB, NZ, NY, NX), 1.0, 6.0, ((1, 64), (2, 4)))
    coeffs = normal_values(keys[2], (KB,), 0.02, 0.3125, (), jnp.float32)
    rhs = normal_values(keys[3], (NZ, NY, NX), 1.0, 8.0, ((0, 64), (1, 4)), jnp.float32)
    kappa = jnp.clip(jnp.exp(math.log(4.0) - 2.0794415 * jax.random.uniform(keys[4], (NZ, NY, NX), jnp.float32) ** block_scale(keys[4], (NZ, NY, NX), ((0, 64), (1, 4)), -0.2, 0.2)), 0.5, 4.0)
    offsets = plant(jax.random.randint(keys[5], (NZ, NY, NX // BLK), 0, SK), jax.random.fold_in(keys[5], 1), 0, SK - 1).astype(jnp.int32)
    flips = plant(jax.random.randint(keys[6], (NZ, NY, NX // BLK), 0, 2), jax.random.fold_in(keys[6], 1), 0, 1).astype(jnp.int32)
    return {"iterate": iterate, "basis": basis, "coeffs": coeffs, "rhs": rhs, "kappa": kappa, "offsets": offsets, "flips": flips}


def apply_operator(upad, kpad):
    field = upad[1:-1, 1:-1, :]
    coef = kpad[1:-1, 1:-1, :]
    total = 0.05 * field
    neighbours = [(upad[2:, 1:-1, :], kpad[2:, 1:-1, :]), (upad[:-2, 1:-1, :], kpad[:-2, 1:-1, :]), (upad[1:-1, 2:, :], kpad[1:-1, 2:, :]), (upad[1:-1, :-2, :], kpad[1:-1, :-2, :])]
    zero_col = jnp.zeros_like(field[:, :, :1])
    neighbours.append((jnp.concatenate([field[:, :, 1:], zero_col], 2), jnp.concatenate([coef[:, :, 1:], zero_col], 2)))
    neighbours.append((jnp.concatenate([zero_col, field[:, :, :-1]], 2), jnp.concatenate([zero_col, coef[:, :, :-1]], 2)))
    for other, kother in neighbours:
        total = total + 0.5 * (coef + kother) * (field - other)
    return total

def reference(iterate, basis, coeffs, rhs, kappa, offsets, flips):
    coeff_b = lax.optimization_barrier(coeffs.astype(jnp.bfloat16)).astype(jnp.float32)

    def accumulate(index, acc):
        vector = lax.dynamic_index_in_dim(basis, index, 0, keepdims=False).astype(jnp.float32)
        return acc + coeff_b[index] * vector
    new_iterate = lax.fori_loop(0, KB, accumulate, iterate)
    widths = ((1, 1), (1, 1), (0, 0))
    operated = apply_operator(jnp.pad(new_iterate, widths), jnp.pad(kappa, widths))
    residual = rhs - operated
    blocks = residual.reshape(-1, BLK)
    signs = (2 * flips - 1).astype(jnp.float32).reshape(-1, 1)
    rows = (offsets.reshape(-1, 1) + jnp.arange(BLK, dtype=jnp.int32)[None, :]) % SK
    sketch = jax.ops.segment_sum((blocks * signs).reshape(-1), rows.reshape(-1).astype(jnp.int32), num_segments=SK)
    sketch_unit = sketch / jnp.sqrt(jnp.mean(sketch * sketch) + 1e-06)
    return (new_iterate, residual, sketch_unit)
```

```python
import functools

import jax
import jax.numpy as jnp
from jax import lax
from jax.experimental import pallas as pl
from jax.experimental.pallas import tpu as pltpu
from jax.sharding import Mesh
from jax.sharding import PartitionSpec as P

SK = 2048
BLK = 128
ROWS = SK // BLK
GZ = ("z", "x", "core")
CHUNK = 16


def stream_kernel(coeff_ref, iterate_ref, basis_ref, new_ref, same_ref, cross_ref, ye_ref, yo_ref, held, splat, sems):
    kb, nz, ny, nx = basis_ref.shape
    pieces = ny // CHUNK
    copies = []
    for i in range(pieces):
        rows = pl.ds(i * CHUNK, CHUNK)
        copies.append(pltpu.make_async_copy(basis_ref.at[:, :, rows, :], held.at[i], sems.at[i]))
    for copy in copies:
        copy.start()
    core = lax.axis_index("core")
    odd = lax.rem(lax.axis_index("gy"), 2)
    rounded = coeff_ref[...].astype(jnp.bfloat16).astype(jnp.float32)
    for k in range(kb):
        splat[k] = jnp.broadcast_to(rounded[:, k : k + 1], (8, BLK))
    for i in range(pieces):
        copies[i].wait()

        @pl.loop(0, nx // BLK)
        def _(j, i=i):
            lanes = pl.ds(pl.multiple_of(j * BLK, BLK), BLK)
            rows = pl.ds(i * CHUNK, CHUNK)
            acc = [iterate_ref[z, rows, lanes] for z in range(nz)]
            for k in range(kb):
                scale = splat[k]
                scale = jnp.concatenate([scale] * (CHUNK // 8), 0)
                for z in range(nz):
                    acc[z] = acc[z] + scale * held[i, k, z, :, lanes].astype(jnp.float32)
            for z in range(nz):
                new_ref[z, rows, lanes] = acc[z]
            same_ref[rows, lanes] = jnp.where(core == 0, acc[1], acc[0])
            cross_ref[rows, lanes] = jnp.where(core == 0, acc[0], acc[1])

    for z in range(nz):
        low, high = new_ref[z, 0:1, :], new_ref[z, ny - 1 : ny, :]
        ye_ref[z : z + 1, :] = jnp.where(odd == 0, high, low)
        yo_ref[z : z + 1, :] = jnp.where(odd == 0, low, high)


def update(coeffs, iterate, basis):
    kb, nz, ny, nx = basis.shape
    vmem = pl.BlockSpec(memory_space=pltpu.VMEM)
    plane = jax.ShapeDtypeStruct((ny, nx), jnp.float32)
    row = jax.ShapeDtypeStruct((nz, nx), jnp.float32)
    return pl.pallas_call(
        stream_kernel,
        out_shape=(jax.ShapeDtypeStruct(iterate.shape, jnp.float32), plane, plane, row, row),
        in_specs=[vmem, vmem, pl.BlockSpec(memory_space=pl.ANY)],
        out_specs=(vmem,) * 5,
        scratch_shapes=[
            pltpu.VMEM((ny // CHUNK, kb, nz, CHUNK, nx), jnp.bfloat16),
            pltpu.VMEM((kb, 8, BLK), jnp.float32),
            pltpu.SemaphoreType.DMA((ny // CHUNK,)),
        ],
        compiler_params=pltpu.CompilerParams(vmem_limit_bytes=16 << 20),
        cost_estimate=pl.CostEstimate(flops=2 * basis.size, bytes_accessed=2 * basis.size, transcendentals=0),
        name="update",
    )(coeffs.reshape(1, kb), iterate, basis)


def shifted(value, by, axis):
    return pltpu.roll(value, by % value.shape[axis], axis)


def residual_kernel(
    u_ref, k_ref, rhs_ref, off_ref, flip_ref,
    us_ref, uc_ref, ks_ref, kc_ref, ue_ref, uo_ref, ke_ref, ko_ref,
    res_ref, part_ref,
):
    nz, ny, nx = u_ref.shape
    core = lax.axis_index("core")
    odd = lax.rem(lax.axis_index("gy"), 2)
    lane = lax.broadcasted_iota(jnp.int32, (8, nx), 1)
    line = lax.broadcasted_iota(jnp.int32, (8, nx), 0)
    first, last = lane == 0, lane == nx - 1
    top, bottom = line == 0, line == 7

    def pick(even, same, cross):
        return jnp.where(even, same, cross)

    for z in range(nz):
        lowy_u = pick(odd == 0, uo_ref[z : z + 1, :], ue_ref[z : z + 1, :])
        lowy_k = pick(odd == 0, ko_ref[z : z + 1, :], ke_ref[z : z + 1, :])
        highy_u = pick(odd == 0, ue_ref[z : z + 1, :], uo_ref[z : z + 1, :])
        highy_k = pick(odd == 0, ke_ref[z : z + 1, :], ko_ref[z : z + 1, :])
        for y in range(0, ny, 8):
            rows = slice(y, y + 8)
            u, k = u_ref[z, rows, :], k_ref[z, rows, :]
            total = 0.05 * u
            halo = core == (0 if z else 1)
            uz = pick(halo, us_ref[rows, :], uc_ref[rows, :])
            kz = pick(halo, ks_ref[rows, :], kc_ref[rows, :])
            total = total + 0.5 * (k + kz) * (u - uz)
            total = total + 0.5 * (k + k_ref[1 - z, rows, :]) * (u - u_ref[1 - z, rows, :])
            if y == 0:
                ul = jnp.where(top, lowy_u, shifted(u, 1, 0))
                kl = jnp.where(top, lowy_k, shifted(k, 1, 0))
            else:
                ul, kl = u_ref[z, y - 1 : y + 7, :], k_ref[z, y - 1 : y + 7, :]
            if y == ny - 8:
                uh = jnp.where(bottom, highy_u, shifted(u, -1, 0))
                kh = jnp.where(bottom, highy_k, shifted(k, -1, 0))
            else:
                uh, kh = u_ref[z, y + 1 : y + 9, :], k_ref[z, y + 1 : y + 9, :]
            total = total + 0.5 * (k + kl) * (u - ul)
            total = total + 0.5 * (k + kh) * (u - uh)
            ur = jnp.where(last, 0.0, shifted(u, -1, 1))
            kr = jnp.where(last, 0.0, shifted(k, -1, 1))
            right = 0.5 * (k + kr) * (u - ur)
            left = jnp.where(first, -0.5 * k * u, shifted(right, 1, 1))
            res_ref[z, rows, :] = rhs_ref[z, rows, :] - (total + (right - left))

    spot = lax.broadcasted_iota(jnp.int32, (ny, BLK), 1)
    slot = lax.broadcasted_iota(jnp.int32, (ROWS, ny), 0)
    whole = jnp.zeros((ROWS, BLK), jnp.float32)
    carry = jnp.zeros((ROWS, BLK), jnp.float32)
    for z in range(nz):
        turned = jnp.transpose(off_ref[z] & (BLK - 1))
        for q in range(nx // BLK):
            by = jnp.broadcast_to(turned[:, q : q + 1], (ny, BLK))
            block = res_ref[z, :, q * BLK : (q + 1) * BLK]
            block = jnp.take_along_axis(block, (spot - by) & (BLK - 1), axis=1)
            high = block.astype(jnp.bfloat16)
            low = (block - high.astype(jnp.float32)).astype(jnp.bfloat16)
            sign = (2 * flip_ref[z, q : q + 1, :] - 1).astype(jnp.float32)
            row = jnp.right_shift(off_ref[z, q : q + 1, :], 7)
            place = jnp.where(slot == row, sign, 0.0).astype(jnp.bfloat16)
            here = spot >= by
            none = jnp.zeros_like(high)
            for term in (high, low):
                pair = jnp.concatenate([jnp.where(here, term, none), jnp.where(here, none, term)], 1)
                got = jnp.dot(place, pair, preferred_element_type=jnp.float32)
                whole = whole + got[:, :BLK]
                carry = carry + got[:, BLK:]
    sketch = whole + jnp.concatenate([carry[ROWS - 1 :], carry[: ROWS - 1]], 0)
    for m in range(part_ref.shape[0]):
        part_ref[m] = sketch


def residual_and_sketch(members, *arrays):
    vmem = pl.BlockSpec(memory_space=pltpu.VMEM)
    u = arrays[0]
    return pl.pallas_call(
        residual_kernel,
        out_shape=(
            jax.ShapeDtypeStruct(u.shape, jnp.float32),
            jax.ShapeDtypeStruct((members, ROWS, BLK), jnp.float32),
        ),
        in_specs=[vmem] * len(arrays),
        out_specs=(vmem, vmem),
        compiler_params=pltpu.CompilerParams(vmem_limit_bytes=16 << 20),
        cost_estimate=pl.CostEstimate(flops=60 * u.size, bytes_accessed=8 * u.size, transcendentals=0),
        name="residual",
    )(*arrays)


def scale_kernel(parts_ref, out_ref):
    sketch = jnp.sum(parts_ref[...], axis=0)
    mean = jnp.sum(sketch * sketch) * (1.0 / SK)
    out_ref[...] = sketch / jnp.sqrt(jnp.broadcast_to(mean + 1e-06, sketch.shape))


def scaled(parts):
    vmem = pl.BlockSpec(memory_space=pltpu.VMEM)
    return pl.pallas_call(
        scale_kernel,
        out_shape=jax.ShapeDtypeStruct((ROWS, BLK), jnp.float32),
        in_specs=[vmem],
        out_specs=vmem,
        compiler_params=pltpu.CompilerParams(vmem_limit_bytes=4 << 20),
        name="scaled",
    )(parts)


def shards(sizes, iterate, basis, coeffs, rhs, kappa, offsets, flips):
    gz = sizes["z"] * sizes["x"] * sizes["core"]
    gy = sizes["gy"]
    core = lax.axis_index("core")
    odd = lax.rem(lax.axis_index("gy"), 2)
    same = [(i, i ^ 1) for i in range(gz)]
    cross = [(i, i + 1) for i in range(1, gz - 1, 2)] + [(i + 1, i) for i in range(1, gz - 1, 2)]
    even_y = [(i, i ^ 1) for i in range(gy)]
    odd_y = [(i, i + 1) for i in range(1, gy - 1, 2)] + [(i + 1, i) for i in range(1, gy - 1, 2)]

    k_cross = lax.ppermute(jnp.where(core == 0, kappa[0], kappa[1]), GZ, cross)
    k_same = lax.ppermute(jnp.where(core == 0, kappa[1], kappa[0]), GZ, same)
    k_even = lax.ppermute(jnp.where(odd == 0, kappa[:, -1], kappa[:, 0]), "gy", even_y)
    k_odd = lax.ppermute(jnp.where(odd == 0, kappa[:, 0], kappa[:, -1]), "gy", odd_y)

    u, u_same, u_cross, u_even, u_odd = update(coeffs, iterate, basis)
    u_cross = lax.ppermute(u_cross, GZ, cross)
    u_same = lax.ppermute(u_same, GZ, same)
    u_even = lax.ppermute(u_even, "gy", even_y)
    u_odd = lax.ppermute(u_odd, "gy", odd_y)

    plane_of = ("x", "gy")
    line_of = ("z", "core")
    members = sizes["x"] * sizes["gy"]
    others = sizes["z"] * sizes["core"]
    residual, part = residual_and_sketch(
        members, u, kappa, rhs, jnp.swapaxes(offsets, 1, 2), jnp.swapaxes(flips, 1, 2),
        u_same, u_cross, k_same, k_cross, u_even, u_odd, k_even, k_odd,
    )
    part = lax.all_to_all(part, plane_of, 0, 0)
    part = jnp.broadcast_to(jnp.sum(part, 0), (others, ROWS, BLK))
    part = lax.all_to_all(part, line_of, 0, 0)
    return u, residual, scaled(part).reshape(SK)


def build(mesh, outer):
    gy = mesh.shape["gy"]
    finer = Mesh(mesh.devices.reshape(*outer, gy), (*GZ, "gy"))
    sizes = dict(finer.shape)
    field = P(GZ, "gy", None)
    return jax.shard_map(
        functools.partial(shards, sizes),
        mesh=finer,
        in_specs=(field, P(None, GZ, "gy", None), P(), field, field, field, field),
        out_specs=(field, field, P()),
        check_vma=False,
    )


def solution(mesh):
    return build(mesh, (mesh.shape["gz"] // 8, 4, 2))
```

```python
import functools

import jax
import jax.numpy as jnp
from jax import lax
from jax.experimental import pallas as pl
from jax.experimental.pallas import tpu as pltpu
from jax.sharding import Mesh
from jax.sharding import PartitionSpec as P


SK = 2048
BLK = 128
ROWS = SK // BLK
GROUP = 4
GZ = ("z", "x", "core")
HBM = pl.BlockSpec(memory_space=pltpu.HBM)
VMEM = pl.BlockSpec(memory_space=pltpu.VMEM)


def f32(*shape):
    return jax.ShapeDtypeStruct(shape, jnp.float32)


def parities():
    return lax.axis_index("core") == 0, lax.rem(lax.axis_index("gy"), 2) == 0


def columns(table):
    return jnp.transpose(table)


def spread(column, q, height):
    return jnp.broadcast_to(column[:, q : q + 1], (height, BLK))


def edge_kernel(k_hbm, off_hbm, flip_hbm, same_ref, cross_ref, even_ref, odd_ref, k_ref, off_ref, flip_ref, sems):
    copies = [
        pltpu.make_async_copy(source, target, sems.at[i])
        for i, (source, target) in enumerate(((k_hbm, k_ref), (off_hbm, off_ref), (flip_hbm, flip_ref)))
    ]
    for copy in copies:
        copy.start()
    for copy in copies:
        copy.wait()
    nz, ny, nx = k_ref.shape
    blocks = nx // BLK
    core0, even = parities()

    def both(low, high):
        return jnp.where(core0, high, low), jnp.where(core0, low, high)

    same_ref[:ny], cross_ref[:ny] = both(k_ref[0], k_ref[1])
    offs = [off_ref[z].astype(jnp.float32) for z in range(nz)]
    signs = [(2 * flip_ref[z] - 1).astype(jnp.float32) for z in range(nz)]
    same_ref[ny:, :ny], cross_ref[ny:, :ny] = both(offs[0], offs[1])
    same_ref[ny:, BLK : BLK + ny], cross_ref[ny:, BLK : BLK + ny] = both(signs[0], signs[1])
    for z in range(nz):
        off_t, sign_t = columns(offs[z]), columns(signs[z])
        for q in range(blocks):
            lanes = slice(q * BLK, (q + 1) * BLK)
            for at, table in ((nz + z, off_t), (2 * nz + z, sign_t)):
                low = jnp.broadcast_to(table[:1, q : q + 1], (1, BLK))
                high = jnp.broadcast_to(table[ny - 1 :, q : q + 1], (1, BLK))
                even_ref[at : at + 1, lanes] = jnp.where(even, high, low)
                odd_ref[at : at + 1, lanes] = jnp.where(even, low, high)
        low, high = k_ref[z, :1, :], k_ref[z, ny - 1 :, :]
        even_ref[z : z + 1, :] = jnp.where(even, high, low)
        odd_ref[z : z + 1, :] = jnp.where(even, low, high)
    rest = slice(3 * nz, 8)
    even_ref[rest, :] = jnp.zeros((8 - 3 * nz, nx), jnp.float32)
    odd_ref[rest, :] = jnp.zeros((8 - 3 * nz, nx), jnp.float32)


def edges(kappa, offsets, flips):
    nz, ny, nx = kappa.shape
    plane, line = f32(ny + 8, nx), f32(8, nx)
    return pl.pallas_call(
        edge_kernel,
        out_shape=(plane, plane, line, line),
        in_specs=[HBM] * 3,
        out_specs=(VMEM,) * 4,
        scratch_shapes=[pltpu.VMEM(v.shape, v.dtype) for v in (kappa, offsets, flips)] + [pltpu.SemaphoreType.DMA((3,))],
        compiler_params=pltpu.CompilerParams(vmem_limit_bytes=8 << 20),
        cost_estimate=pl.CostEstimate(flops=1 << 32, bytes_accessed=1 << 28, transcendentals=0),
        name="edges",
    )(*(pltpu.with_memory_space_constraint(v, pltpu.HBM) for v in (kappa, offsets, flips)))


def shifted(value, by, axis):
    return pltpu.roll(value, by % value.shape[axis], axis)


def main_kernel(
    coeff_ref, iterate_ref, basis_ref, k_ref, rhs_ref, off_ref, flip_ref, same_ref, cross_ref, even_ref, odd_ref,
    out_ref, us_ref, uc_ref, ue_ref, uo_ref, base_ref, wz_ref, wy_ref, part_ref,
    u_ref, splat, hz_ref, hy_ref, sem,
):
    kb, nz, ny, nx = basis_ref.shape
    core0, even = parities()
    rounded = coeff_ref[...].astype(jnp.bfloat16).astype(jnp.float32)
    for k in range(kb):
        splat[k] = jnp.broadcast_to(rounded[:, k : k + 1], (8, BLK))

    @pl.loop(0, ny // 16)
    def _(i):
        rows = pl.ds(pl.multiple_of(i * 16, 16), 16)

        @pl.loop(0, nx // BLK)
        def _(j):
            lanes = pl.ds(pl.multiple_of(j * BLK, BLK), BLK)
            acc = [iterate_ref[z, rows, lanes] for z in range(nz)]
            for k in range(kb):
                scale = jnp.concatenate([splat[k]] * 2, 0)
                for z in range(nz):
                    acc[z] = acc[z] + scale * basis_ref[k, z, rows, lanes].astype(jnp.float32)
            for z in range(nz):
                u_ref[z, rows, lanes] = acc[z]
            us_ref[rows, lanes] = jnp.where(core0, acc[1], acc[0])
            uc_ref[rows, lanes] = jnp.where(core0, acc[0], acc[1])

    store = pltpu.make_async_copy(u_ref, out_ref, sem)
    store.start()

    for z in range(nz):
        low, high = u_ref[z, :1, :], u_ref[z, ny - 1 :, :]
        ue_ref[z : z + 1, :] = jnp.where(even, high, low)
        uo_ref[z : z + 1, :] = jnp.where(even, low, high)

    lane = lax.broadcasted_iota(jnp.int32, (8, nx), 1)
    line = lax.broadcasted_iota(jnp.int32, (8, nx), 0)
    first, last = lane == 0, lane == nx - 1
    low_y = jnp.where(even, odd_ref[...], even_ref[...])
    high_y = jnp.where(even, even_ref[...], odd_ref[...])
    for z in range(nz):
        for y in range(0, ny, 8):
            rows = slice(y, y + 8)
            u, k = u_ref[z, rows, :], k_ref[z, rows, :]
            swap = core0 if z else jnp.logical_not(core0)
            wz = 0.5 * (k + jnp.where(swap, same_ref[rows, :], cross_ref[rows, :]))
            wz_ref[z, rows, :] = wz
            out = wz * u
            hz_ref[z, rows, :] = out
            total = 0.05 * u + out
            total = total + 0.5 * (k + k_ref[1 - z, rows, :]) * (u - u_ref[1 - z, rows, :])
            if y == 0:
                ul, kl = shifted(u, 1, 0), shifted(k, 1, 0)
                ul = jnp.where(line == 0, 0.0, ul)
                kl = jnp.where(line == 0, low_y[z : z + 1, :], kl)
                w = 0.5 * (k + kl)
                wy_ref[z : z + 1, :] = w[:1]
                hy_ref[z : z + 1, :] = (w * u)[:1]
            else:
                ul = u_ref[z, y - 1 : y + 7, :]
                w = 0.5 * (k + k_ref[z, y - 1 : y + 7, :])
            total = total + w * (u - ul)
            if y == ny - 8:
                uh, kh = shifted(u, -1, 0), shifted(k, -1, 0)
                uh = jnp.where(line == 7, 0.0, uh)
                kh = jnp.where(line == 7, high_y[z : z + 1, :], kh)
                w = 0.5 * (k + kh)
                wy_ref[nz + z : nz + z + 1, :] = w[7:]
                hy_ref[nz + z : nz + z + 1, :] = (w * u)[7:]
            else:
                uh = u_ref[z, y + 1 : y + 9, :]
                w = 0.5 * (k + k_ref[z, y + 1 : y + 9, :])
            total = total + w * (u - uh)
            ur = jnp.where(last, 0.0, shifted(u, -1, 1))
            kr = jnp.where(last, 0.0, shifted(k, -1, 1))
            right = 0.5 * (k + kr) * (u - ur)
            left = jnp.where(first, -0.5 * k * u, shifted(right, 1, 1))
            base_ref[z, rows, :] = rhs_ref[z, rows, :] - (total + (right - left))

    blocks = nx // BLK
    sums = []

    def place(offs, signs):
        slot = lax.broadcasted_iota(jnp.int32, (ROWS, offs.shape[1]), 0)
        return jnp.where(slot == jnp.right_shift(offs, 7), signs, 0.0).astype(jnp.bfloat16)

    def turn(block, by):
        spot = lax.broadcasted_iota(jnp.int32, block.shape, 1)
        block = jnp.take_along_axis(block, (spot - by) & (BLK - 1), axis=1)
        block = jnp.concatenate([jnp.where(spot >= by, block, 0.0), jnp.where(spot >= by, 0.0, block)], 1)
        high = block.astype(jnp.bfloat16)
        return high, (block - high.astype(jnp.float32)).astype(jnp.bfloat16)

    def add(spots, terms):
        at = jnp.concatenate(spots * 2, 1)
        values = jnp.concatenate([t[0] for t in terms] + [t[1] for t in terms], 0)
        sums.append(jnp.dot(at, values, preferred_element_type=jnp.float32))

    for z in range(nz):
        swap = core0 if z else jnp.logical_not(core0)
        theirs = jnp.where(swap, same_ref[ny:, : 2 * BLK], cross_ref[ny:, : 2 * BLK])
        mine = (2 * flip_ref[z] - 1).astype(jnp.float32)
        for source, offs, signs in (
            (base_ref, off_ref[z], mine),
            (hz_ref, theirs[:, :ny].astype(jnp.int32), theirs[:, BLK : BLK + ny]),
        ):
            turned = columns(offs & (BLK - 1))
            for start in range(0, blocks, GROUP):
                group = range(start, start + GROUP)
                at = place(
                    jnp.concatenate([offs[q : q + 1, :] for q in group], 1),
                    jnp.concatenate([signs[q : q + 1, :] for q in group], 1),
                )
                add([at], [turn(source[z, :, q * BLK : (q + 1) * BLK], spread(turned, q, ny)) for q in group])

    hy_ref[2 * nz :, :] = jnp.zeros((16 - 2 * nz, nx), jnp.float32)
    unused = jnp.zeros((16 - 2 * nz, nx), jnp.float32)
    y_offs = jnp.concatenate([low_y[nz : 2 * nz], high_y[nz : 2 * nz], unused], 0).astype(jnp.int32)
    y_signs = jnp.concatenate([low_y[2 * nz : 3 * nz], high_y[2 * nz : 3 * nz], unused], 0)
    spots, terms = [], []
    for q in range(blocks):
        lanes = slice(q * BLK, (q + 1) * BLK)
        offs, signs = y_offs[:, lanes], y_signs[:, lanes]
        spots.append(place(jnp.transpose(offs[:, :1]), jnp.transpose(signs[:, :1])))
        terms.append(turn(hy_ref[:, lanes], offs & (BLK - 1)))
    add(spots, terms)

    got = sum(sums[1:], sums[0])
    carry = got[:, BLK:]
    part_ref[...] = got[:, :BLK] + jnp.concatenate([carry[ROWS - 1 :], carry[: ROWS - 1]], 0)
    store.wait()


def main(coeffs, iterate, basis, kappa, rhs, *rest):
    kb, nz, ny, nx = basis.shape
    field = f32(nz, ny, nx)
    return pl.pallas_call(
        main_kernel,
        out_shape=(
            field, f32(ny, nx), f32(ny, nx), f32(nz, nx), f32(nz, nx), field, field, f32(2 * nz, nx), f32(ROWS, BLK),
        ),
        in_specs=[VMEM] * 11,
        out_specs=(pl.BlockSpec(memory_space=pl.ANY),) + (VMEM,) * 8,
        scratch_shapes=[
            pltpu.VMEM((nz, ny, nx), jnp.float32),
            pltpu.VMEM((kb, 8, BLK), jnp.float32),
            pltpu.VMEM((nz, ny, nx), jnp.float32),
            pltpu.VMEM((16, nx), jnp.float32),
            pltpu.SemaphoreType.DMA,
        ],
        compiler_params=pltpu.CompilerParams(vmem_limit_bytes=24 << 20),
        cost_estimate=pl.CostEstimate(flops=4 * basis.size, bytes_accessed=2 * basis.size, transcendentals=0),
        name="main",
    )(coeffs.reshape(1, kb), iterate, basis, kappa, rhs, *rest)


def halo_kernel(base_ref, wz_ref, wy_ref, us_ref, uc_ref, ue_ref, uo_ref, res_ref):
    nz, ny, _ = base_ref.shape
    core0, even = parities()
    low_y = jnp.where(even, uo_ref[...], ue_ref[...])
    high_y = jnp.where(even, ue_ref[...], uo_ref[...])
    for z in range(nz):
        swap = core0 if z else jnp.logical_not(core0)
        for y in range(0, ny, 8):
            rows = slice(y, y + 8)
            value = base_ref[z, rows, :] + wz_ref[z, rows, :] * jnp.where(swap, us_ref[rows, :], uc_ref[rows, :])
            res_ref[z, rows, :] = value
        res_ref[z, :1, :] += wy_ref[z : z + 1, :] * low_y[z : z + 1, :]
        res_ref[z, ny - 1 :, :] += wy_ref[nz + z : nz + z + 1, :] * high_y[z : z + 1, :]


def with_halo(base, *rest):
    return pl.pallas_call(
        halo_kernel,
        out_shape=f32(*base.shape),
        in_specs=[VMEM] * 7,
        out_specs=VMEM,
        compiler_params=pltpu.CompilerParams(vmem_limit_bytes=8 << 20),
        cost_estimate=pl.CostEstimate(flops=1 << 20, bytes_accessed=2 << 20, transcendentals=0),
        name="halo",
    )(base, *rest)


def scale_kernel(*refs):
    sketch = refs[0][...]
    for ref in refs[1:-1]:
        sketch = sketch + ref[...]
    mean = jnp.sum(sketch * sketch) * (1.0 / SK)
    refs[-1][...] = sketch / jnp.sqrt(jnp.broadcast_to(mean + 1e-06, sketch.shape))


def scaled(*parts):
    return pl.pallas_call(
        scale_kernel,
        out_shape=f32(ROWS, BLK),
        in_specs=[VMEM] * len(parts),
        out_specs=VMEM,
        compiler_params=pltpu.CompilerParams(vmem_limit_bytes=4 << 20),
        name="scaled",
    )(*parts)


def pairs_from(first, count):
    ups = [(i, i + 1) for i in range(first, count - 1, 2)]
    return ups + [(b, a) for a, b in ups]


def rounds(count):
    if count == 1:
        return []
    if count == 8:
        third = [(5, 0), (0, 5), (4, 1), (1, 4), (7, 2), (2, 7), (6, 3), (3, 6)]
        second = [(i, (i - 2) % 8) for i in range(0, 8, 2)] + [(i, (i + 2) % 8) for i in range(1, 8, 2)]
        near = [(i, (i + 1) % 8) for i in range(1, 8, 2)]
        near = near + [(b, a) for a, b in near]
        return [[pairs_from(0, 8)], [third, second, near]]
    order = sorted(range(1, count), key=lambda d: -min(d, count - d))
    return [[[(i, (i + d) % count) for i in range(count)] for d in order]]


def shards(sizes, iterate, basis, coeffs, rhs, kappa, offsets, flips):
    gz = sizes["z"] * sizes["x"] * sizes["core"]
    gy = sizes["gy"]
    ways = ((GZ, pairs_from(0, gz)), (GZ, pairs_from(1, gz)), ("gy", pairs_from(0, gy)), ("gy", pairs_from(1, gy)))

    def swap(values):
        return [lax.ppermute(v, axis, pairs) for v, (axis, pairs) in zip(values, ways)]

    offsets, flips = jnp.swapaxes(offsets, 1, 2), jnp.swapaxes(flips, 1, 2)
    static = swap(edges(kappa, offsets, flips))
    u, *sends, base, wz, wy, part = main(coeffs, iterate, basis, kappa, rhs, offsets, flips, *static)
    terms = [part]
    for axis in ("core", "gy", "x", "z"):
        for step in rounds(sizes[axis]):
            value = sum(terms[1:], terms[0])
            terms = [value] + [lax.ppermute(value, axis, pairs) for pairs in step]
    residual = with_halo(base, wz, wy, *swap(sends))
    return u, residual, scaled(*terms).reshape(SK)


def build(mesh, outer):
    gy = mesh.shape["gy"]
    finer = Mesh(mesh.devices.reshape(*outer, gy), (*GZ, "gy"))
    sizes = dict(finer.shape)
    field = P(GZ, "gy", None)
    return jax.shard_map(
        functools.partial(shards, sizes),
        mesh=finer,
        in_specs=(field, P(None, GZ, "gy", None), P(), field, field, field, field),
        out_specs=(field, field, P()),
        check_vma=False,
    )


def solution(mesh):
    return build(mesh, (mesh.shape["gz"] // 8, 4, 2))
```

```python
import functools

import jax
import jax.numpy as jnp
from jax import lax
from jax.experimental import pallas as pl
from jax.experimental.pallas import tpu as pltpu
from jax.sharding import Mesh
from jax.sharding import PartitionSpec as P


SK = 2048
BLK = 128
ROWS = SK // BLK
GROUP = 4
GZ = ("z", "x", "core")
HBM = pl.BlockSpec(memory_space=pltpu.HBM)
VMEM = pl.BlockSpec(memory_space=pltpu.VMEM)


def f32(*shape):
    return jax.ShapeDtypeStruct(shape, jnp.float32)


def parities():
    return lax.axis_index("core") == 0, lax.rem(lax.axis_index("gy"), 2) == 0


def columns(table):
    return jnp.transpose(table)


def spread(column, q, height):
    return jnp.broadcast_to(column[:, q : q + 1], (height, BLK))


def edge_kernel(k_hbm, off_hbm, flip_hbm, same_ref, cross_ref, even_ref, odd_ref, k_ref, off_ref, flip_ref, sems):
    copies = [
        pltpu.make_async_copy(source, target, sems.at[i])
        for i, (source, target) in enumerate(((k_hbm, k_ref), (off_hbm, off_ref), (flip_hbm, flip_ref)))
    ]
    for copy in copies:
        copy.start()
    for copy in copies:
        copy.wait()
    nz, ny, nx = k_ref.shape
    blocks = nx // BLK
    core0, even = parities()

    def both(low, high):
        return jnp.where(core0, high, low), jnp.where(core0, low, high)

    same_ref[:ny], cross_ref[:ny] = both(k_ref[0], k_ref[1])
    offs = [off_ref[z].astype(jnp.float32) for z in range(nz)]
    signs = [(2 * flip_ref[z] - 1).astype(jnp.float32) for z in range(nz)]
    same_ref[ny:, :ny], cross_ref[ny:, :ny] = both(offs[0], offs[1])
    same_ref[ny:, BLK : BLK + ny], cross_ref[ny:, BLK : BLK + ny] = both(signs[0], signs[1])
    for z in range(nz):
        off_t, sign_t = columns(offs[z]), columns(signs[z])
        for q in range(blocks):
            lanes = slice(q * BLK, (q + 1) * BLK)
            for at, table in ((nz + z, off_t), (2 * nz + z, sign_t)):
                low = jnp.broadcast_to(table[:1, q : q + 1], (1, BLK))
                high = jnp.broadcast_to(table[ny - 1 :, q : q + 1], (1, BLK))
                even_ref[at : at + 1, lanes] = jnp.where(even, high, low)
                odd_ref[at : at + 1, lanes] = jnp.where(even, low, high)
        low, high = k_ref[z, :1, :], k_ref[z, ny - 1 :, :]
        even_ref[z : z + 1, :] = jnp.where(even, high, low)
        odd_ref[z : z + 1, :] = jnp.where(even, low, high)
    rest = slice(3 * nz, 8)
    even_ref[rest, :] = jnp.zeros((8 - 3 * nz, nx), jnp.float32)
    odd_ref[rest, :] = jnp.zeros((8 - 3 * nz, nx), jnp.float32)


def edges(kappa, offsets, flips):
    nz, ny, nx = kappa.shape
    plane, line = f32(ny + 8, nx), f32(8, nx)
    return pl.pallas_call(
        edge_kernel,
        out_shape=(plane, plane, line, line),
        in_specs=[HBM] * 3,
        out_specs=(VMEM,) * 4,
        scratch_shapes=[pltpu.VMEM(v.shape, v.dtype) for v in (kappa, offsets, flips)] + [pltpu.SemaphoreType.DMA((3,))],
        compiler_params=pltpu.CompilerParams(vmem_limit_bytes=8 << 20),
        cost_estimate=pl.CostEstimate(flops=1 << 32, bytes_accessed=1 << 28, transcendentals=0),
        name="edges",
    )(*(pltpu.with_memory_space_constraint(v, pltpu.HBM) for v in (kappa, offsets, flips)))


def update_kernel(coeff_ref, iterate_ref, basis_ref, u_ref, splat):
    kb, nz, ny, nx = basis_ref.shape
    rounded = coeff_ref[...].astype(jnp.bfloat16).astype(jnp.float32)
    for k in range(kb):
        splat[k] = jnp.broadcast_to(rounded[:, k : k + 1], (8, BLK))

    @pl.loop(0, ny // 16)
    def _(i):
        rows = pl.ds(pl.multiple_of(i * 16, 16), 16)

        @pl.loop(0, nx // (2 * BLK))
        def _(j):
            lanes = [pl.ds(pl.multiple_of((2 * j + h) * BLK, BLK), BLK) for h in range(2)]
            spots = [(z, rows, part) for z in range(nz) for part in lanes]
            acc = [iterate_ref[spot] for spot in spots]
            for k in range(kb):
                scale = jnp.concatenate([splat[k]] * 2, 0)
                for n, spot in enumerate(spots):
                    acc[n] = acc[n] + scale * basis_ref[(k, *spot)].astype(jnp.float32)
            for n, spot in enumerate(spots):
                u_ref[spot] = acc[n]


def update(coeffs, iterate, basis):
    kb = basis.shape[0]
    return pl.pallas_call(
        update_kernel,
        out_shape=f32(*iterate.shape),
        in_specs=[VMEM] * 3,
        out_specs=VMEM,
        scratch_shapes=[pltpu.VMEM((kb, 8, BLK), jnp.float32)],
        compiler_params=pltpu.CompilerParams(vmem_limit_bytes=16 << 20),
        cost_estimate=pl.CostEstimate(flops=1 << 24, bytes_accessed=2 * basis.size, transcendentals=0),
        name="update",
    )(coeffs.reshape(1, kb), iterate, basis)


def lane_gather(values, index):
    numbers = lax.GatherDimensionNumbers(
        offset_dims=(),
        collapsed_slice_dims=(1,),
        start_index_map=(1,),
        operand_batching_dims=(0,),
        start_indices_batching_dims=(0,),
    )
    return lax.gather(values, index[..., None], numbers, (1, 1), mode=lax.GatherScatterMode.PROMISE_IN_BOUNDS)


def sketch_kernel(
    u_ref, k_ref, rhs_ref, off_ref, flip_ref, same_ref, cross_ref, even_ref, odd_ref,
    out_ref, us_ref, uc_ref, ue_ref, uo_ref, base_ref, wz_ref, wy_ref,
    hz_ref, hy_ref, sem,
):
    nz, ny, nx = u_ref.shape
    core0, even = parities()
    blocks = nx // BLK
    store = pltpu.make_async_copy(u_ref, out_ref, sem)
    store.start()

    for z in range(nz):
        low, high = u_ref[z, :1, :], u_ref[z, ny - 1 :, :]
        ue_ref[z : z + 1, :] = jnp.where(even, high, low)
        uo_ref[z : z + 1, :] = jnp.where(even, low, high)

    lane = lax.broadcasted_iota(jnp.int32, (8, BLK), 1)
    line = lax.broadcasted_iota(jnp.int32, (8, BLK), 0)
    low_y = jnp.where(even, odd_ref[...], even_ref[...])
    high_y = jnp.where(even, even_ref[...], odd_ref[...])
    cells = [(z, q) for z in range(nz) for q in range(blocks)]

    def lanes(q):
        return slice(q * BLK, (q + 1) * BLK)

    def tile(ref, y):
        return {(z, q): ref[z, y : y + 8, lanes(q)] for z, q in cells}

    def up(tiles):
        return {c: pltpu.roll(t, 7, 0) for c, t in tiles.items()}

    u, k = tile(u_ref, 0), tile(k_ref, 0)
    u_up, k_up = up(u), up(k)
    below = None
    for y in range(0, ny, 8):
        rows = slice(y, y + 8)
        if y + 8 < ny:
            u_next, k_next = tile(u_ref, y + 8), tile(k_ref, y + 8)
            u_next_up, k_next_up = up(u_next), up(k_next)
        else:
            u_next = k_next = None
            u_next_up = {c: 0.0 for c in cells}
            k_next_up = {(z, q): high_y[z : z + 1, lanes(q)] for z, q in cells}
        between = {q: (k[0, q] + k[1, q]) * (u[0, q] - u[1, q]) for q in range(blocks)}
        above = {}
        for z in range(nz):
            swap = core0 if z else jnp.logical_not(core0)
            u_right = {q: pltpu.roll(u[z, q], BLK - 1, 1) for q in range(blocks)}
            k_right = {q: pltpu.roll(k[z, q], BLK - 1, 1) for q in range(blocks)}
            u_right[blocks] = k_right[blocks] = 0.0
            left = None
            for q in range(blocks):
                c = (z, q)
                pair = k[c] + jnp.where(swap, same_ref[rows, lanes(q)], cross_ref[rows, lanes(q)])
                wz = 0.5 * pair
                wz_ref[z, rows, lanes(q)] = wz
                hz_ref[z, rows, lanes(q)] = wz * u[c]
                total = pair * u[c]
                total = total - between[q] if z else total + between[q]
                flow = (k[c] + jnp.where(line == 7, k_next_up[c], k_up[c])) * (
                    u[c] - jnp.where(line == 7, u_next_up[c], u_up[c])
                )
                above[c] = pltpu.roll(flow, 1, 0)
                if y == 0:
                    edge = k[c] + low_y[z : z + 1, lanes(q)]
                    wy_ref[z : z + 1, lanes(q)] = 0.5 * edge[:1]
                    edge = edge * u[c]
                    hy_ref[z : z + 1, lanes(q)] = 0.5 * edge[:1]
                    before = -edge
                else:
                    before = below[c]
                if y == ny - 8:
                    edge = k[c] + high_y[z : z + 1, lanes(q)]
                    wy_ref[nz + z : nz + z + 1, lanes(q)] = 0.5 * edge[7:]
                    hy_ref[nz + z : nz + z + 1, lanes(q)] = 0.5 * (edge * u[c])[7:]
                total = total + (flow - jnp.where(line == 0, before, above[c]))
                flow = (k[c] + jnp.where(lane == BLK - 1, k_right[q + 1], k_right[q])) * (
                    u[c] - jnp.where(lane == BLK - 1, u_right[q + 1], u_right[q])
                )
                turned = pltpu.roll(flow, 1, 1)
                before = -k[c] * u[c] if q == 0 else left
                total = total + (flow - jnp.where(lane == 0, before, turned))
                left = turned
                base_ref[z, rows, lanes(q)] = (rhs_ref[z, rows, lanes(q)] - 0.05 * u[c]) - 0.5 * total
        below = above
        u, k, u_up, k_up = u_next, k_next, u_next_up, k_next_up

    for y in range(0, ny, 8):
        rows = slice(y, y + 8)
        us_ref[rows, :] = jnp.where(core0, u_ref[1, rows, :], u_ref[0, rows, :])
        uc_ref[rows, :] = jnp.where(core0, u_ref[0, rows, :], u_ref[1, rows, :])

    sums = []

    def place(offs, signs):
        slot = lax.broadcasted_iota(jnp.int32, (ROWS, offs.shape[1]), 0)
        return jnp.where(slot == jnp.right_shift(offs, 7), signs, 0.0).astype(jnp.bfloat16)

    def turn(block, by):
        spot = lax.broadcasted_iota(jnp.int32, block.shape, 1)
        here = spot >= by
        block = lane_gather(block, (spot - by) & (BLK - 1))
        high = block.astype(jnp.bfloat16)
        low = (block - high.astype(jnp.float32)).astype(jnp.bfloat16)
        none = jnp.zeros_like(high)
        return [jnp.concatenate([jnp.where(here, t, none), jnp.where(here, none, t)], 1) for t in (high, low)]

    def add(spots, terms):
        at = jnp.concatenate(spots * 2, 1)
        values = jnp.concatenate([t[0] for t in terms] + [t[1] for t in terms], 0)
        sums.append(jnp.dot(at, values, preferred_element_type=jnp.float32))

    for z in range(nz):
        swap = core0 if z else jnp.logical_not(core0)
        theirs = jnp.where(swap, same_ref[ny:, : 2 * BLK], cross_ref[ny:, : 2 * BLK])
        mine = (2 * flip_ref[z] - 1).astype(jnp.float32)
        for source, offs, signs in (
            (base_ref, off_ref[z], mine),
            (hz_ref, theirs[:, :ny].astype(jnp.int32), theirs[:, BLK : BLK + ny]),
        ):
            turned = columns(offs & (BLK - 1))
            for start in range(0, blocks, GROUP):
                group = range(start, start + GROUP)
                at = place(
                    jnp.concatenate([offs[q : q + 1, :] for q in group], 1),
                    jnp.concatenate([signs[q : q + 1, :] for q in group], 1),
                )
                add([at], [turn(source[z, :, lanes(q)], spread(turned, q, ny)) for q in group])

    hy_ref[2 * nz :, :] = jnp.zeros((16 - 2 * nz, nx), jnp.float32)
    unused = jnp.zeros((16 - 2 * nz, nx), jnp.float32)
    y_offs = jnp.concatenate([low_y[nz : 2 * nz], high_y[nz : 2 * nz], unused], 0).astype(jnp.int32)
    y_signs = jnp.concatenate([low_y[2 * nz : 3 * nz], high_y[2 * nz : 3 * nz], unused], 0)
    spots, terms = [], []
    for q in range(blocks):
        offs, signs = y_offs[:, lanes(q)], y_signs[:, lanes(q)]
        spots.append(place(jnp.transpose(offs[:, :1]), jnp.transpose(signs[:, :1])))
        terms.append(turn(hy_ref[:, lanes(q)], offs & (BLK - 1)))
    add(spots, terms)

    got = sum(sums[1:], sums[0])
    carry = got[:, BLK:]
    part = got[:, :BLK] + jnp.concatenate([carry[ROWS - 1 :], carry[: ROWS - 1]], 0)
    us_ref[ny:, :] = jnp.zeros((8, nx), jnp.float32)
    for m in range(ROWS):
        at = ny + m // blocks
        us_ref[at : at + 1, lanes(m % blocks)] = part[m : m + 1]
    store.wait()


def sketch(u, *rest):
    nz, ny, nx = u.shape
    field = f32(nz, ny, nx)
    return pl.pallas_call(
        sketch_kernel,
        out_shape=(field, f32(ny + 8, nx), f32(ny, nx), f32(nz, nx), f32(nz, nx), field, field, f32(2 * nz, nx)),
        in_specs=[VMEM] * 9,
        out_specs=(pl.BlockSpec(memory_space=pl.ANY),) + (VMEM,) * 7,
        scratch_shapes=[
            pltpu.VMEM((nz, ny, nx), jnp.float32),
            pltpu.VMEM((16, nx), jnp.float32),
            pltpu.SemaphoreType.DMA,
        ],
        compiler_params=pltpu.CompilerParams(vmem_limit_bytes=16 << 20),
        cost_estimate=pl.CostEstimate(flops=1 << 24, bytes_accessed=16 << 20, transcendentals=0),
        name="sketch",
    )(u, *rest)


def halo_kernel(base_ref, wz_ref, wy_ref, us_ref, uc_ref, ue_ref, uo_ref, res_ref):
    nz, ny, _ = base_ref.shape
    core0, even = parities()
    spot = lax.axis_index("gy")
    low_y = jnp.where(even, uo_ref[...], ue_ref[...])
    low_y = jnp.where(spot == 0, 0.0, low_y)
    high_y = jnp.where(even, ue_ref[...], uo_ref[...])
    high_y = jnp.where(spot == lax.axis_size("gy") - 1, 0.0, high_y)
    for z in range(nz):
        swap = core0 if z else jnp.logical_not(core0)
        for y in range(0, ny, 8):
            rows = slice(y, y + 8)
            value = base_ref[z, rows, :] + wz_ref[z, rows, :] * jnp.where(swap, us_ref[rows, :], uc_ref[rows, :])
            res_ref[z, rows, :] = value
        res_ref[z, :1, :] += wy_ref[z : z + 1, :] * low_y[nz + z : nz + z + 1, :]
        res_ref[z, ny - 1 :, :] += wy_ref[nz + z : nz + z + 1, :] * high_y[nz + z : nz + z + 1, :]


def with_halo(base, *rest):
    return pl.pallas_call(
        halo_kernel,
        out_shape=f32(*base.shape),
        in_specs=[VMEM] * 7,
        out_specs=VMEM,
        compiler_params=pltpu.CompilerParams(vmem_limit_bytes=8 << 20),
        cost_estimate=pl.CostEstimate(flops=1 << 20, bytes_accessed=2 << 20, transcendentals=0),
        name="halo",
    )(base, *rest)


def scale_kernel(*refs):
    sketch = refs[0][...]
    for ref in refs[1:-1]:
        sketch = sketch + ref[...]
    mean = jnp.sum(sketch * sketch) * (1.0 / SK)
    unit = sketch / jnp.sqrt(jnp.broadcast_to(mean + 1e-06, sketch.shape))
    wide = sketch.shape[1] // BLK
    for m in range(ROWS):
        refs[-1][m : m + 1, :] = unit[m // wide : m // wide + 1, m % wide * BLK : (m % wide + 1) * BLK]


def scaled(*parts):
    return pl.pallas_call(
        scale_kernel,
        out_shape=f32(ROWS, BLK),
        in_specs=[VMEM] * len(parts),
        out_specs=VMEM,
        compiler_params=pltpu.CompilerParams(vmem_limit_bytes=4 << 20),
        name="scaled",
    )(*parts)


def pairs_from(first, count, ring=False):
    ups = [(i, (i + 1) % count) for i in range(first, count if ring else count - 1, 2)]
    return ups + [(b, a) for a, b in ups]


def rounds(count):
    if count == 1:
        return []
    if count == 8:
        third = [(5, 0), (0, 5), (4, 1), (1, 4), (7, 2), (2, 7), (6, 3), (3, 6)]
        second = [(i, (i - 2) % 8) for i in range(0, 8, 2)] + [(i, (i + 2) % 8) for i in range(1, 8, 2)]
        return [[pairs_from(0, 8)], [third, second, pairs_from(1, 8, ring=True)]]
    return [[pairs_from(first, count, ring=True)] for first in range(count // 2)]


def shards(sizes, iterate, basis, coeffs, rhs, kappa, offsets, flips):
    gz = sizes["z"] * sizes["x"] * sizes["core"]
    gy = sizes["gy"]
    nz, ny, _ = kappa.shape
    same, cross = pairs_from(0, gz), pairs_from(1, gz)
    even, odd = pairs_from(0, gy), pairs_from(1, gy)

    offsets, flips = jnp.swapaxes(offsets, 1, 2), jnp.swapaxes(flips, 1, 2)
    k_same, k_cross, k_even, k_odd = edges(kappa, offsets, flips)
    k_cross = lax.ppermute(k_cross, GZ, cross)
    k_same = lax.ppermute(k_same, GZ, same)
    k_even = lax.ppermute(k_even, "gy", even)
    k_odd = lax.ppermute(k_odd, "gy", odd)
    u = update(coeffs, iterate, basis)
    u_out, u_same, u_cross, u_even, u_odd, base, wz, wy = sketch(
        u, kappa, rhs, offsets, flips, k_same, k_cross, k_even, k_odd
    )
    got = lax.ppermute(u_same, GZ, same)
    value = u_same[ny : ny + 2] + got[ny : ny + 2]
    u_same = got
    lines = []
    for pairs, line in ((even, u_even), (pairs_from(1, gy, ring=True), u_odd)):
        got = lax.ppermute(jnp.concatenate([value, line], 0), "gy", pairs)
        value = value + got[:2]
        lines.append(got)
    terms = [value]
    for axis in ("x", "z"):
        for step in rounds(sizes[axis]):
            value = sum(terms[1:], terms[0])
            if axis == "z" and len(step) == 1:
                u_cross, value = lax.optimization_barrier((u_cross, value))
            terms = [value] + [lax.ppermute(value, axis, pairs) for pairs in step]
    u_cross = lax.ppermute(u_cross, GZ, cross)
    residual = with_halo(base, wz, wy, u_same, u_cross, *lines)
    return u_out, residual, scaled(*terms).reshape(SK)


def build(mesh, outer):
    gy = mesh.shape["gy"]
    finer = Mesh(mesh.devices.reshape(*outer, gy), (*GZ, "gy"))
    sizes = dict(finer.shape)
    field = P(GZ, "gy", None)
    return jax.shard_map(
        functools.partial(shards, sizes),
        mesh=finer,
        in_specs=(field, P(None, GZ, "gy", None), P(), field, field, field, field),
        out_specs=(field, field, P()),
        check_vma=False,
    )


def solution(mesh):
    return build(mesh, (mesh.shape["gz"] // 8, 4, 2))
```

```python
import functools

import jax
import jax.numpy as jnp
from jax import lax
from jax.experimental import pallas as pl
from jax.experimental.pallas import tpu as pltpu
from jax.sharding import Mesh
from jax.sharding import PartitionSpec as P


SK = 2048
BLK = 128
ROWS = SK // BLK
GROUP = 4
GZ = ("z", "x", "core")
HBM = pl.BlockSpec(memory_space=pltpu.HBM)
VMEM = pl.BlockSpec(memory_space=pltpu.VMEM)


def f32(*shape):
    return jax.ShapeDtypeStruct(shape, jnp.float32)


def parities():
    return lax.axis_index("core") == 0, lax.rem(lax.axis_index("gy"), 2) == 0


def columns(table):
    return jnp.transpose(table)


def spread(column, q, height):
    return jnp.broadcast_to(column[:, q : q + 1], (height, BLK))


def edge_kernel(k_hbm, off_hbm, flip_hbm, same_ref, cross_ref, even_ref, odd_ref, k_ref, off_ref, flip_ref, sems):
    copies = [
        pltpu.make_async_copy(source, target, sems.at[i])
        for i, (source, target) in enumerate(((k_hbm, k_ref), (off_hbm, off_ref), (flip_hbm, flip_ref)))
    ]
    for copy in copies:
        copy.start()
    for copy in copies:
        copy.wait()
    nz, ny, nx = k_ref.shape
    blocks = nx // BLK
    core0, even = parities()

    def both(low, high):
        return jnp.where(core0, high, low), jnp.where(core0, low, high)

    same_ref[:ny], cross_ref[:ny] = both(k_ref[0], k_ref[1])
    offs = [off_ref[z].astype(jnp.float32) for z in range(nz)]
    signs = [(2 * flip_ref[z] - 1).astype(jnp.float32) for z in range(nz)]
    same_ref[ny:, :ny], cross_ref[ny:, :ny] = both(offs[0], offs[1])
    same_ref[ny:, BLK : BLK + ny], cross_ref[ny:, BLK : BLK + ny] = both(signs[0], signs[1])
    for z in range(nz):
        off_t, sign_t = columns(offs[z]), columns(signs[z])
        for q in range(blocks):
            lanes = slice(q * BLK, (q + 1) * BLK)
            for at, table in ((nz + z, off_t), (2 * nz + z, sign_t)):
                low = jnp.broadcast_to(table[:1, q : q + 1], (1, BLK))
                high = jnp.broadcast_to(table[ny - 1 :, q : q + 1], (1, BLK))
                even_ref[at : at + 1, lanes] = jnp.where(even, high, low)
                odd_ref[at : at + 1, lanes] = jnp.where(even, low, high)
        low, high = k_ref[z, :1, :], k_ref[z, ny - 1 :, :]
        even_ref[z : z + 1, :] = jnp.where(even, high, low)
        odd_ref[z : z + 1, :] = jnp.where(even, low, high)
    rest = slice(3 * nz, 8)
    even_ref[rest, :] = jnp.zeros((8 - 3 * nz, nx), jnp.float32)
    odd_ref[rest, :] = jnp.zeros((8 - 3 * nz, nx), jnp.float32)


def edges(kappa, offsets, flips):
    _, ny, nx = kappa.shape
    plane, line = f32(ny + 8, nx), f32(8, nx)
    return pl.pallas_call(
        edge_kernel,
        out_shape=(plane, plane, line, line),
        in_specs=[HBM] * 3,
        out_specs=(VMEM,) * 4,
        scratch_shapes=[pltpu.VMEM(v.shape, v.dtype) for v in (kappa, offsets, flips)] + [pltpu.SemaphoreType.DMA((3,))],
        compiler_params=pltpu.CompilerParams(vmem_limit_bytes=8 << 20),
        cost_estimate=pl.CostEstimate(flops=1 << 32, bytes_accessed=1 << 28, transcendentals=0),
        name="edges",
    )(*(pltpu.with_memory_space_constraint(v, pltpu.HBM) for v in (kappa, offsets, flips)))


def update_kernel(coeff_ref, iterate_ref, basis_ref, u_ref, uc_ref, splat):
    kb, nz, ny, nx = basis_ref.shape
    core0, _ = parities()
    rounded = coeff_ref[...].astype(jnp.bfloat16).astype(jnp.float32)
    for k in range(kb):
        splat[k] = jnp.broadcast_to(rounded[:, k : k + 1], (8, BLK))

    @pl.loop(0, ny // 16)
    def _(i):
        rows = pl.ds(pl.multiple_of(i * 16, 16), 16)

        @pl.loop(0, nx // (2 * BLK))
        def _(j):
            lanes = [pl.ds(pl.multiple_of((2 * j + h) * BLK, BLK), BLK) for h in range(2)]
            spots = [(z, rows, part) for z in range(nz) for part in lanes]
            acc = [iterate_ref[spot] for spot in spots]
            for k in range(kb):
                scale = jnp.concatenate([splat[k]] * 2, 0)
                for n, spot in enumerate(spots):
                    acc[n] = acc[n] + scale * basis_ref[(k, *spot)].astype(jnp.float32)
            for n, spot in enumerate(spots):
                u_ref[spot] = acc[n]
            for n, part in enumerate(lanes):
                uc_ref[rows, part] = jnp.where(core0, acc[n], acc[len(lanes) + n])


def update(coeffs, iterate, basis):
    kb = basis.shape[0]
    return pl.pallas_call(
        update_kernel,
        out_shape=(f32(*iterate.shape), f32(*iterate.shape[1:])),
        in_specs=[VMEM] * 3,
        out_specs=(VMEM, VMEM),
        scratch_shapes=[pltpu.VMEM((kb, 8, BLK), jnp.float32)],
        compiler_params=pltpu.CompilerParams(vmem_limit_bytes=16 << 20),
        cost_estimate=pl.CostEstimate(flops=1 << 24, bytes_accessed=2 * basis.size, transcendentals=0),
        name="update",
    )(coeffs.reshape(1, kb), iterate, basis)


def lane_gather(values, index):
    numbers = lax.GatherDimensionNumbers(
        offset_dims=(),
        collapsed_slice_dims=(1,),
        start_index_map=(1,),
        operand_batching_dims=(0,),
        start_indices_batching_dims=(0,),
    )
    return lax.gather(values, index[..., None], numbers, (1, 1), mode=lax.GatherScatterMode.PROMISE_IN_BOUNDS)


def sketch_kernel(
    u_ref, k_ref, rhs_ref, off_ref, flip_ref, same_ref, cross_ref, even_ref, odd_ref,
    out_ref, us_ref, ue_ref, uo_ref, base_ref, wz_ref, wy_ref,
    hz_ref, hy_ref, sem,
):
    nz, ny, nx = u_ref.shape
    core0, even = parities()
    blocks = nx // BLK
    store = pltpu.make_async_copy(u_ref, out_ref, sem)
    store.start()

    for z in range(nz):
        low, high = u_ref[z, :1, :], u_ref[z, ny - 1 :, :]
        ue_ref[z : z + 1, :] = jnp.where(even, high, low)
        uo_ref[z : z + 1, :] = jnp.where(even, low, high)

    lane = lax.broadcasted_iota(jnp.int32, (8, BLK), 1)
    line = lax.broadcasted_iota(jnp.int32, (8, BLK), 0)
    low_y = jnp.where(even, odd_ref[...], even_ref[...])
    high_y = jnp.where(even, even_ref[...], odd_ref[...])
    cells = [(z, q) for z in range(nz) for q in range(blocks)]

    def lanes(q):
        return slice(q * BLK, (q + 1) * BLK)

    def tile(ref, y):
        return {(z, q): ref[z, y : y + 8, lanes(q)] for z, q in cells}

    def up(tiles):
        return {c: pltpu.roll(t, 7, 0) for c, t in tiles.items()}

    u, k = tile(u_ref, 0), tile(k_ref, 0)
    u_up, k_up = up(u), up(k)
    below = None
    for y in range(0, ny, 8):
        rows = slice(y, y + 8)
        if y + 8 < ny:
            u_next, k_next = tile(u_ref, y + 8), tile(k_ref, y + 8)
            u_next_up, k_next_up = up(u_next), up(k_next)
        else:
            u_next = k_next = None
            u_next_up = {c: 0.0 for c in cells}
            k_next_up = {(z, q): high_y[z : z + 1, lanes(q)] for z, q in cells}
        between = {q: (k[0, q] + k[1, q]) * (u[0, q] - u[1, q]) for q in range(blocks)}
        above = {}
        for z in range(nz):
            swap = core0 if z else jnp.logical_not(core0)
            u_right = {q: pltpu.roll(u[z, q], BLK - 1, 1) for q in range(blocks)}
            k_right = {q: pltpu.roll(k[z, q], BLK - 1, 1) for q in range(blocks)}
            u_right[blocks] = k_right[blocks] = 0.0
            left = None
            for q in range(blocks):
                c = (z, q)
                pair = k[c] + jnp.where(swap, same_ref[rows, lanes(q)], cross_ref[rows, lanes(q)])
                wz = 0.5 * pair
                wz_ref[z, rows, lanes(q)] = wz
                hz_ref[z, rows, lanes(q)] = wz * u[c]
                total = pair * u[c]
                total = total - between[q] if z else total + between[q]
                flow = (k[c] + jnp.where(line == 7, k_next_up[c], k_up[c])) * (
                    u[c] - jnp.where(line == 7, u_next_up[c], u_up[c])
                )
                above[c] = pltpu.roll(flow, 1, 0)
                if y == 0:
                    edge = k[c] + low_y[z : z + 1, lanes(q)]
                    wy_ref[z : z + 1, lanes(q)] = 0.5 * edge[:1]
                    edge = edge * u[c]
                    hy_ref[z : z + 1, lanes(q)] = 0.5 * edge[:1]
                    before = -edge
                else:
                    before = below[c]
                if y == ny - 8:
                    edge = k[c] + high_y[z : z + 1, lanes(q)]
                    wy_ref[nz + z : nz + z + 1, lanes(q)] = 0.5 * edge[7:]
                    hy_ref[nz + z : nz + z + 1, lanes(q)] = 0.5 * (edge * u[c])[7:]
                total = total + (flow - jnp.where(line == 0, before, above[c]))
                flow = (k[c] + jnp.where(lane == BLK - 1, k_right[q + 1], k_right[q])) * (
                    u[c] - jnp.where(lane == BLK - 1, u_right[q + 1], u_right[q])
                )
                turned = pltpu.roll(flow, 1, 1)
                before = -k[c] * u[c] if q == 0 else left
                total = total + (flow - jnp.where(lane == 0, before, turned))
                left = turned
                base_ref[z, rows, lanes(q)] = (rhs_ref[z, rows, lanes(q)] - 0.05 * u[c]) - 0.5 * total
        below = above
        u, k, u_up, k_up = u_next, k_next, u_next_up, k_next_up

    for y in range(0, ny, 8):
        rows = slice(y, y + 8)
        us_ref[rows, :] = jnp.where(core0, u_ref[1, rows, :], u_ref[0, rows, :])

    sums = []

    def place(offs, signs):
        slot = lax.broadcasted_iota(jnp.int32, (ROWS, offs.shape[1]), 0)
        return jnp.where(slot == jnp.right_shift(offs, 7), signs, 0.0).astype(jnp.bfloat16)

    def turn(block, by):
        spot = lax.broadcasted_iota(jnp.int32, block.shape, 1)
        here = spot >= by
        block = lane_gather(block, (spot - by) & (BLK - 1))
        high = block.astype(jnp.bfloat16)
        low = (block - high.astype(jnp.float32)).astype(jnp.bfloat16)
        none = jnp.zeros_like(high)
        return [jnp.concatenate([jnp.where(here, t, none), jnp.where(here, none, t)], 1) for t in (high, low)]

    def add(spots, terms):
        at = jnp.concatenate(spots * 2, 1)
        values = jnp.concatenate([t[0] for t in terms] + [t[1] for t in terms], 0)
        sums.append(jnp.dot(at, values, preferred_element_type=jnp.float32))

    for z in range(nz):
        swap = core0 if z else jnp.logical_not(core0)
        theirs = jnp.where(swap, same_ref[ny:, : 2 * BLK], cross_ref[ny:, : 2 * BLK])
        mine = (2 * flip_ref[z] - 1).astype(jnp.float32)
        for source, offs, signs in (
            (base_ref, off_ref[z], mine),
            (hz_ref, theirs[:, :ny].astype(jnp.int32), theirs[:, BLK : BLK + ny]),
        ):
            turned = columns(offs & (BLK - 1))
            for start in range(0, blocks, GROUP):
                group = range(start, start + GROUP)
                at = place(
                    jnp.concatenate([offs[q : q + 1, :] for q in group], 1),
                    jnp.concatenate([signs[q : q + 1, :] for q in group], 1),
                )
                add([at], [turn(source[z, :, lanes(q)], spread(turned, q, ny)) for q in group])

    hy_ref[2 * nz :, :] = jnp.zeros((16 - 2 * nz, nx), jnp.float32)
    unused = jnp.zeros((16 - 2 * nz, nx), jnp.float32)
    y_offs = jnp.concatenate([low_y[nz : 2 * nz], high_y[nz : 2 * nz], unused], 0).astype(jnp.int32)
    y_signs = jnp.concatenate([low_y[2 * nz : 3 * nz], high_y[2 * nz : 3 * nz], unused], 0)
    spots, terms = [], []
    for q in range(blocks):
        offs, signs = y_offs[:, lanes(q)], y_signs[:, lanes(q)]
        spots.append(place(jnp.transpose(offs[:, :1]), jnp.transpose(signs[:, :1])))
        terms.append(turn(hy_ref[:, lanes(q)], offs & (BLK - 1)))
    add(spots, terms)

    got = sum(sums[1:], sums[0])
    carry = got[:, BLK:]
    part = got[:, :BLK] + jnp.concatenate([carry[ROWS - 1 :], carry[: ROWS - 1]], 0)
    us_ref[ny:, :] = jnp.zeros((8, nx), jnp.float32)
    for m in range(ROWS):
        at = ny + m // blocks
        us_ref[at : at + 1, lanes(m % blocks)] = part[m : m + 1]
    store.wait()


def sketch(u, *rest):
    nz, ny, nx = u.shape
    field = f32(nz, ny, nx)
    return pl.pallas_call(
        sketch_kernel,
        out_shape=(field, f32(ny + 8, nx), f32(nz, nx), f32(nz, nx), field, field, f32(2 * nz, nx)),
        in_specs=[VMEM] * 9,
        out_specs=(pl.BlockSpec(memory_space=pl.ANY),) + (VMEM,) * 6,
        scratch_shapes=[
            pltpu.VMEM((nz, ny, nx), jnp.float32),
            pltpu.VMEM((16, nx), jnp.float32),
            pltpu.SemaphoreType.DMA,
        ],
        compiler_params=pltpu.CompilerParams(vmem_limit_bytes=16 << 20),
        cost_estimate=pl.CostEstimate(flops=1 << 24, bytes_accessed=16 << 20, transcendentals=0),
        name="sketch",
    )(u, *rest)


def halo_kernel(base_ref, wz_ref, wy_ref, us_ref, uc_ref, ue_ref, uo_ref, res_ref):
    nz, ny, _ = base_ref.shape
    core0, even = parities()
    low_y = jnp.where(even, uo_ref[...], ue_ref[...])
    high_y = jnp.where(even, ue_ref[...], uo_ref[...])
    for z in range(nz):
        swap = core0 if z else jnp.logical_not(core0)
        for y in range(0, ny, 8):
            rows = slice(y, y + 8)
            value = base_ref[z, rows, :] + wz_ref[z, rows, :] * jnp.where(swap, us_ref[rows, :], uc_ref[rows, :])
            res_ref[z, rows, :] = value
        res_ref[z, :1, :] += wy_ref[z : z + 1, :] * low_y[nz + z : nz + z + 1, :]
        res_ref[z, ny - 1 :, :] += wy_ref[nz + z : nz + z + 1, :] * high_y[nz + z : nz + z + 1, :]


def with_halo(base, *rest):
    return pl.pallas_call(
        halo_kernel,
        out_shape=f32(*base.shape),
        in_specs=[VMEM] * 7,
        out_specs=VMEM,
        compiler_params=pltpu.CompilerParams(vmem_limit_bytes=8 << 20),
        cost_estimate=pl.CostEstimate(flops=1 << 20, bytes_accessed=2 << 20, transcendentals=0),
        name="halo",
    )(base, *rest)


def scale_kernel(*refs):
    sketch = refs[0][...]
    for ref in refs[1:-1]:
        sketch = sketch + ref[...]
    mean = jnp.sum(sketch * sketch) * (1.0 / SK)
    unit = sketch / jnp.sqrt(jnp.broadcast_to(mean + 1e-06, sketch.shape))
    wide = sketch.shape[1] // BLK
    for m in range(ROWS):
        refs[-1][m : m + 1, :] = unit[m // wide : m // wide + 1, m % wide * BLK : (m % wide + 1) * BLK]


def scaled(*parts):
    return pl.pallas_call(
        scale_kernel,
        out_shape=f32(ROWS, BLK),
        in_specs=[VMEM] * len(parts),
        out_specs=VMEM,
        compiler_params=pltpu.CompilerParams(vmem_limit_bytes=4 << 20),
        name="scaled",
    )(*parts)


def both_ways(pairs):
    return pairs + [(b, a) for a, b in pairs]


def pairs_from(first, count):
    return both_ways([(i, i + 1) for i in range(first, count - 1, 2)])


def rounds(count):
    pairs = {"pair": pairs_from(0, count)}
    if count == 2:
        return [pairs]
    if count == 4:
        return [pairs, {"far": [(2, 0), (1, 3)], "near": pairs_from(1, count)}]
    third = both_ways([(0, 5), (1, 4), (2, 7), (3, 6)])
    second = [(i, (i - 2) % 8) for i in range(0, 8, 2)] + [(i, (i + 2) % 8) for i in range(1, 8, 2)]
    first = both_ways([(i, (i + 1) % 8) for i in range(1, 8, 2)])
    return [pairs, {"third": third, "second": second, "first": first}]


def shards(sizes, *arrays):
    return cycle_end(sizes, *arrays)


def cycle_end(sizes, iterate, basis, coeffs, rhs, kappa, offsets, flips):
    gz = sizes["z"] * sizes["x"] * sizes["core"]
    gy = sizes["gy"]
    _, ny, _ = kappa.shape
    same, cross = pairs_from(0, gz), pairs_from(1, gz)
    even, odd = pairs_from(0, gy), pairs_from(1, gy)

    offsets, flips = jnp.swapaxes(offsets, 1, 2), jnp.swapaxes(flips, 1, 2)
    k_same, k_cross, k_even, k_odd = edges(kappa, offsets, flips)
    k_cross = lax.ppermute(k_cross, GZ, cross)
    k_same = lax.ppermute(k_same, GZ, same)
    k_even = lax.ppermute(k_even, "gy", even)
    k_odd = lax.ppermute(k_odd, "gy", odd)
    u, u_cross = update(coeffs, iterate, basis)
    u_cross = lax.ppermute(u_cross, GZ, cross)
    u_out, u_same, u_even, u_odd, base, wz, wy = sketch(u, kappa, rhs, offsets, flips, k_same, k_cross, k_even, k_odd)
    got = lax.ppermute(u_same, GZ, same)
    value = u_same[ny : ny + 2] + got[ny : ny + 2]
    u_same = got
    u_even = lax.ppermute(jnp.concatenate([value, u_even], 0), "gy", even)
    value = value + u_even[:2]
    far = lax.ppermute(value, "gy", rounds(gy)[1]["far"])
    u_odd = lax.ppermute(jnp.concatenate([value, u_odd], 0), "gy", odd)
    value = value + far + u_odd[:2]
    terms = [value]
    for axis in ("x", "z"):
        for step in rounds(sizes[axis]) if sizes[axis] > 1 else ():
            value = sum(terms[1:], terms[0])
            terms = [value] + [lax.ppermute(value, axis, pairs) for pairs in step.values()]
    residual = with_halo(base, wz, wy, u_same, u_cross, u_even, u_odd)
    return u_out, residual, scaled(*terms).reshape(SK)


def build(mesh, outer):
    gy = mesh.shape["gy"]
    finer = Mesh(mesh.devices.reshape(*outer, gy), (*GZ, "gy"))
    sizes = dict(finer.shape)
    field = P(GZ, "gy", None)
    return jax.shard_map(
        functools.partial(shards, sizes),
        mesh=finer,
        in_specs=(field, P(None, GZ, "gy", None), P(), field, field, field, field),
        out_specs=(field, field, P()),
        check_vma=False,
    )


def solution(mesh):
    return build(mesh, (mesh.shape["gz"] // 8, 4, 2))
```

```python
import functools

import jax
import jax.numpy as jnp
from jax import lax
from jax.experimental import pallas as pl
from jax.experimental.pallas import tpu as pltpu
from jax.sharding import Mesh
from jax.sharding import PartitionSpec as P


SK = 2048
BLK = 128
ROWS = SK // BLK
STEP = 16
WAYS = BLK // STEP
GROUP = 4
GZ = ("z", "x", "core")
HBM = pl.BlockSpec(memory_space=pltpu.HBM)
VMEM = pl.BlockSpec(memory_space=pltpu.VMEM)


def f32(*shape):
    return jax.ShapeDtypeStruct(shape, jnp.float32)


def parities():
    return lax.axis_index("core") == 0, lax.rem(lax.axis_index("gy"), 2) == 0


def columns(table):
    return jnp.transpose(table)


def spread(column, q, height):
    return jnp.broadcast_to(column[:, q : q + 1], (height, BLK))


def edge_kernel(k_hbm, off_hbm, flip_hbm, same_ref, cross_ref, even_ref, odd_ref, k_ref, off_ref, flip_ref, sems):
    copies = [
        pltpu.make_async_copy(source, target, sems.at[i])
        for i, (source, target) in enumerate(((k_hbm, k_ref), (off_hbm, off_ref), (flip_hbm, flip_ref)))
    ]
    for copy in copies:
        copy.start()
    for copy in copies:
        copy.wait()
    nz, ny, nx = k_ref.shape
    blocks = nx // BLK
    core0, even = parities()

    def both(low, high):
        return jnp.where(core0, high, low), jnp.where(core0, low, high)

    same_ref[:ny], cross_ref[:ny] = both(k_ref[0], k_ref[1])
    offs = [off_ref[z].astype(jnp.float32) for z in range(nz)]
    signs = [(2 * flip_ref[z] - 1).astype(jnp.float32) for z in range(nz)]
    same_ref[ny:, :ny], cross_ref[ny:, :ny] = both(offs[0], offs[1])
    same_ref[ny:, BLK : BLK + ny], cross_ref[ny:, BLK : BLK + ny] = both(signs[0], signs[1])
    for z in range(nz):
        off_t, sign_t = columns(offs[z]), columns(signs[z])
        for q in range(blocks):
            lanes = slice(q * BLK, (q + 1) * BLK)
            for at, table in ((nz + z, off_t), (2 * nz + z, sign_t)):
                low = jnp.broadcast_to(table[:1, q : q + 1], (1, BLK))
                high = jnp.broadcast_to(table[ny - 1 :, q : q + 1], (1, BLK))
                even_ref[at : at + 1, lanes] = jnp.where(even, high, low)
                odd_ref[at : at + 1, lanes] = jnp.where(even, low, high)
        low, high = k_ref[z, :1, :], k_ref[z, ny - 1 :, :]
        even_ref[z : z + 1, :] = jnp.where(even, high, low)
        odd_ref[z : z + 1, :] = jnp.where(even, low, high)
    rest = slice(3 * nz, 8)
    even_ref[rest, :] = jnp.zeros((8 - 3 * nz, nx), jnp.float32)
    odd_ref[rest, :] = jnp.zeros((8 - 3 * nz, nx), jnp.float32)


def edges(kappa, offsets, flips):
    _, ny, nx = kappa.shape
    plane, line = f32(ny + 8, nx), f32(8, nx)
    return pl.pallas_call(
        edge_kernel,
        out_shape=(plane, plane, line, line),
        in_specs=[HBM] * 3,
        out_specs=(VMEM,) * 4,
        scratch_shapes=[pltpu.VMEM(v.shape, v.dtype) for v in (kappa, offsets, flips)] + [pltpu.SemaphoreType.DMA((3,))],
        compiler_params=pltpu.CompilerParams(vmem_limit_bytes=8 << 20),
        cost_estimate=pl.CostEstimate(flops=1 << 32, bytes_accessed=1 << 28, transcendentals=0),
        name="edges",
    )(*(pltpu.with_memory_space_constraint(v, pltpu.HBM) for v in (kappa, offsets, flips)))


def update_kernel(coeff_ref, iterate_ref, basis_ref, u_ref, uc_ref, splat):
    kb, nz, ny, nx = basis_ref.shape
    core0, _ = parities()
    rounded = coeff_ref[...].astype(jnp.bfloat16).astype(jnp.float32)
    for k in range(kb):
        splat[k] = jnp.broadcast_to(rounded[:, k : k + 1], (8, BLK))

    @pl.loop(0, ny // 16)
    def _(i):
        rows = pl.ds(pl.multiple_of(i * 16, 16), 16)

        @pl.loop(0, nx // (2 * BLK))
        def _(j):
            lanes = [pl.ds(pl.multiple_of((2 * j + h) * BLK, BLK), BLK) for h in range(2)]
            spots = [(z, rows, part) for z in range(nz) for part in lanes]
            acc = [iterate_ref[spot] for spot in spots]
            for k in range(kb):
                scale = jnp.concatenate([splat[k]] * 2, 0)
                for n, spot in enumerate(spots):
                    acc[n] = acc[n] + scale * basis_ref[(k, *spot)].astype(jnp.float32)
            for n, spot in enumerate(spots):
                u_ref[spot] = acc[n]
            for n, part in enumerate(lanes):
                uc_ref[rows, part] = jnp.where(core0, acc[n], acc[len(lanes) + n])


def update(coeffs, iterate, basis):
    kb = basis.shape[0]
    return pl.pallas_call(
        update_kernel,
        out_shape=(f32(*iterate.shape), f32(*iterate.shape[1:])),
        in_specs=[VMEM] * 3,
        out_specs=(VMEM, VMEM),
        scratch_shapes=[pltpu.VMEM((kb, 8, BLK), jnp.float32)],
        compiler_params=pltpu.CompilerParams(vmem_limit_bytes=16 << 20),
        cost_estimate=pl.CostEstimate(flops=1 << 24, bytes_accessed=2 * basis.size, transcendentals=0),
        name="update",
    )(coeffs.reshape(1, kb), iterate, basis)


def sketch_kernel(
    u_ref, k_ref, rhs_ref, off_ref, flip_ref, same_ref, cross_ref, even_ref, odd_ref,
    out_ref, us_ref, ue_ref, uo_ref, base_ref, wz_ref, wy_ref,
    hz_ref, hy_ref, sem,
):
    nz, ny, nx = u_ref.shape
    core0, even = parities()
    blocks = nx // BLK
    store = pltpu.make_async_copy(u_ref, out_ref, sem)
    store.start()

    for z in range(nz):
        low, high = u_ref[z, :1, :], u_ref[z, ny - 1 :, :]
        ue_ref[z : z + 1, :] = jnp.where(even, high, low)
        uo_ref[z : z + 1, :] = jnp.where(even, low, high)

    lane = lax.broadcasted_iota(jnp.int32, (8, BLK), 1)
    line = lax.broadcasted_iota(jnp.int32, (8, BLK), 0)
    low_y = jnp.where(even, odd_ref[...], even_ref[...])
    high_y = jnp.where(even, even_ref[...], odd_ref[...])
    cells = [(z, q) for z in range(nz) for q in range(blocks)]

    def lanes(q):
        return slice(q * BLK, (q + 1) * BLK)

    def tile(ref, y):
        return {(z, q): ref[z, y : y + 8, lanes(q)] for z, q in cells}

    def up(tiles):
        return {c: pltpu.roll(t, 7, 0) for c, t in tiles.items()}

    u, k = tile(u_ref, 0), tile(k_ref, 0)
    u_up, k_up = up(u), up(k)
    below = None
    for y in range(0, ny, 8):
        rows = slice(y, y + 8)
        if y + 8 < ny:
            u_next, k_next = tile(u_ref, y + 8), tile(k_ref, y + 8)
            u_next_up, k_next_up = up(u_next), up(k_next)
        else:
            u_next = k_next = None
            u_next_up = {c: 0.0 for c in cells}
            k_next_up = {(z, q): high_y[z : z + 1, lanes(q)] for z, q in cells}
        between = {q: (k[0, q] + k[1, q]) * (u[0, q] - u[1, q]) for q in range(blocks)}
        above = {}
        for z in range(nz):
            swap = core0 if z else jnp.logical_not(core0)
            u_right = {q: pltpu.roll(u[z, q], BLK - 1, 1) for q in range(blocks)}
            k_right = {q: pltpu.roll(k[z, q], BLK - 1, 1) for q in range(blocks)}
            u_right[blocks] = k_right[blocks] = 0.0
            left = None
            for q in range(blocks):
                c = (z, q)
                pair = k[c] + jnp.where(swap, same_ref[rows, lanes(q)], cross_ref[rows, lanes(q)])
                wz = 0.5 * pair
                wz_ref[z, rows, lanes(q)] = wz
                hz_ref[z, rows, lanes(q)] = wz * u[c]
                total = pair * u[c]
                total = total - between[q] if z else total + between[q]
                flow = (k[c] + jnp.where(line == 7, k_next_up[c], k_up[c])) * (
                    u[c] - jnp.where(line == 7, u_next_up[c], u_up[c])
                )
                above[c] = pltpu.roll(flow, 1, 0)
                if y == 0:
                    edge = k[c] + low_y[z : z + 1, lanes(q)]
                    wy_ref[z : z + 1, lanes(q)] = 0.5 * edge[:1]
                    edge = edge * u[c]
                    hy_ref[z : z + 1, lanes(q)] = 0.5 * edge[:1]
                    before = -edge
                else:
                    before = below[c]
                if y == ny - 8:
                    edge = k[c] + high_y[z : z + 1, lanes(q)]
                    wy_ref[nz + z : nz + z + 1, lanes(q)] = 0.5 * edge[7:]
                    hy_ref[nz + z : nz + z + 1, lanes(q)] = 0.5 * (edge * u[c])[7:]
                total = total + (flow - jnp.where(line == 0, before, above[c]))
                flow = (k[c] + jnp.where(lane == BLK - 1, k_right[q + 1], k_right[q])) * (
                    u[c] - jnp.where(lane == BLK - 1, u_right[q + 1], u_right[q])
                )
                turned = pltpu.roll(flow, 1, 1)
                before = -k[c] * u[c] if q == 0 else left
                total = total + (flow - jnp.where(lane == 0, before, turned))
                left = turned
                base_ref[z, rows, lanes(q)] = (rhs_ref[z, rows, lanes(q)] - 0.05 * u[c]) - 0.5 * total
        below = above
        u, k, u_up, k_up = u_next, k_next, u_next_up, k_next_up

    for y in range(0, ny, 8):
        rows = slice(y, y + 8)
        us_ref[rows, :] = jnp.where(core0, u_ref[1, rows, :], u_ref[0, rows, :])

    sums = []

    def place(offs, signs):
        slot = lax.broadcasted_iota(jnp.int32, (WAYS * ROWS, offs.shape[1]), 0)
        at = (jnp.right_shift(offs, 4) & (WAYS - 1)) * ROWS + jnp.right_shift(offs, 7)
        return jnp.where(slot == at, signs, 0.0).astype(jnp.bfloat16)

    def turn(block, by):
        spot = lax.broadcasted_iota(jnp.int32, block.shape, 1)
        here = spot >= by
        for shift in (1, 2, 4, 8):
            block = jnp.where((by & shift) != 0, pltpu.roll(block, shift, 1), block)
        high = block.astype(jnp.bfloat16)
        low = (block - high.astype(jnp.float32)).astype(jnp.bfloat16)
        none = jnp.zeros_like(high)
        return [jnp.concatenate([jnp.where(here, t, none), jnp.where(here, none, t)], 1) for t in (high, low)]

    def add(spots, terms):
        at = jnp.concatenate(spots * 2, 1)
        values = jnp.concatenate([t[0] for t in terms] + [t[1] for t in terms], 0)
        sums.append(jnp.dot(at, values, preferred_element_type=jnp.float32))

    for z in range(nz):
        swap = core0 if z else jnp.logical_not(core0)
        theirs = jnp.where(swap, same_ref[ny:, : 2 * BLK], cross_ref[ny:, : 2 * BLK])
        mine = (2 * flip_ref[z] - 1).astype(jnp.float32)
        for source, offs, signs in (
            (base_ref, off_ref[z], mine),
            (hz_ref, theirs[:, :ny].astype(jnp.int32), theirs[:, BLK : BLK + ny]),
        ):
            turned = columns(offs & (STEP - 1))
            for start in range(0, blocks, GROUP):
                group = range(start, start + GROUP)
                at = place(
                    jnp.concatenate([offs[q : q + 1, :] for q in group], 1),
                    jnp.concatenate([signs[q : q + 1, :] for q in group], 1),
                )
                add([at], [turn(source[z, :, lanes(q)], spread(turned, q, ny)) for q in group])

    hy_ref[2 * nz :, :] = jnp.zeros((16 - 2 * nz, nx), jnp.float32)
    unused = jnp.zeros((16 - 2 * nz, nx), jnp.float32)
    y_offs = jnp.concatenate([low_y[nz : 2 * nz], high_y[nz : 2 * nz], unused], 0).astype(jnp.int32)
    y_signs = jnp.concatenate([low_y[2 * nz : 3 * nz], high_y[2 * nz : 3 * nz], unused], 0)
    spots, terms = [], []
    for q in range(blocks):
        offs, signs = y_offs[:, lanes(q)], y_signs[:, lanes(q)]
        spots.append(place(jnp.transpose(offs[:, :1]), jnp.transpose(signs[:, :1])))
        terms.append(turn(hy_ref[:, lanes(q)], offs & (STEP - 1)))
    add(spots, terms)

    wide = sum(sums[1:], sums[0])
    got = wide[:ROWS]
    for way in range(1, WAYS):
        got = got + pltpu.roll(wide[way * ROWS : (way + 1) * ROWS], way * STEP, 1)
    carry = got[:, BLK:]
    part = got[:, :BLK] + jnp.concatenate([carry[ROWS - 1 :], carry[: ROWS - 1]], 0)
    us_ref[ny:, :] = jnp.zeros((8, nx), jnp.float32)
    for m in range(ROWS):
        at = ny + m // blocks
        us_ref[at : at + 1, lanes(m % blocks)] = part[m : m + 1]
    store.wait()


def sketch(u, *rest):
    nz, ny, nx = u.shape
    field = f32(nz, ny, nx)
    return pl.pallas_call(
        sketch_kernel,
        out_shape=(field, f32(ny + 8, nx), f32(nz, nx), f32(nz, nx), field, field, f32(2 * nz, nx)),
        in_specs=[VMEM] * 9,
        out_specs=(pl.BlockSpec(memory_space=pl.ANY),) + (VMEM,) * 6,
        scratch_shapes=[
            pltpu.VMEM((nz, ny, nx), jnp.float32),
            pltpu.VMEM((16, nx), jnp.float32),
            pltpu.SemaphoreType.DMA,
        ],
        compiler_params=pltpu.CompilerParams(vmem_limit_bytes=16 << 20),
        cost_estimate=pl.CostEstimate(flops=1 << 24, bytes_accessed=16 << 20, transcendentals=0),
        name="sketch",
    )(u, *rest)


def halo_kernel(base_ref, wz_ref, wy_ref, us_ref, uc_ref, ue_ref, uo_ref, res_ref):
    nz, ny, _ = base_ref.shape
    core0, even = parities()
    low_y = jnp.where(even, uo_ref[...], ue_ref[...])
    high_y = jnp.where(even, ue_ref[...], uo_ref[...])
    for z in range(nz):
        swap = core0 if z else jnp.logical_not(core0)
        for y in range(0, ny, 8):
            rows = slice(y, y + 8)
            value = base_ref[z, rows, :] + wz_ref[z, rows, :] * jnp.where(swap, us_ref[rows, :], uc_ref[rows, :])
            res_ref[z, rows, :] = value
        res_ref[z, :1, :] += wy_ref[z : z + 1, :] * low_y[z : z + 1, :]
        res_ref[z, ny - 1 :, :] += wy_ref[nz + z : nz + z + 1, :] * high_y[z : z + 1, :]


def with_halo(base, *rest):
    return pl.pallas_call(
        halo_kernel,
        out_shape=f32(*base.shape),
        in_specs=[VMEM] * 7,
        out_specs=VMEM,
        compiler_params=pltpu.CompilerParams(vmem_limit_bytes=8 << 20),
        cost_estimate=pl.CostEstimate(flops=1 << 20, bytes_accessed=2 << 20, transcendentals=0),
        name="halo",
    )(base, *rest)


def scale_kernel(*refs):
    sketch = refs[0][...]
    for ref in refs[1:-1]:
        sketch = sketch + ref[...]
    mean = jnp.sum(sketch * sketch) * (1.0 / SK)
    unit = sketch / jnp.sqrt(jnp.broadcast_to(mean + 1e-06, sketch.shape))
    wide = sketch.shape[1] // BLK
    for m in range(ROWS):
        refs[-1][m : m + 1, :] = unit[m // wide : m // wide + 1, m % wide * BLK : (m % wide + 1) * BLK]


def scaled(*parts):
    return pl.pallas_call(
        scale_kernel,
        out_shape=f32(ROWS, BLK),
        in_specs=[VMEM] * len(parts),
        out_specs=VMEM,
        compiler_params=pltpu.CompilerParams(vmem_limit_bytes=4 << 20),
        name="scaled",
    )(*parts)


def both_ways(pairs):
    return pairs + [(b, a) for a, b in pairs]


def pairs_from(first, count):
    return both_ways([(i, i + 1) for i in range(first, count - 1, 2)])


def rounds(count):
    pairs = {"pair": pairs_from(0, count)}
    if count == 2:
        return [pairs]
    if count == 4:
        return [{f"apart{k}": [(i, i ^ k) for i in range(4)] for k in (3, 2, 1)}]
    third = both_ways([(0, 5), (1, 4), (2, 7), (3, 6)])
    second = [(i, (i - 2) % 8) for i in range(0, 8, 2)] + [(i, (i + 2) % 8) for i in range(1, 8, 2)]
    first = both_ways([(i, (i + 1) % 8) for i in range(1, 8, 2)])
    return [pairs, {"apart3": third, "apart2": second, "apart1": first}]


def shards(sizes, *arrays):
    return cycle_end(sizes, *arrays)


def cycle_end(sizes, iterate, basis, coeffs, rhs, kappa, offsets, flips):
    gz = sizes["z"] * sizes["x"] * sizes["core"]
    gy = sizes["gy"]
    _, ny, _ = kappa.shape
    same, cross = pairs_from(0, gz), pairs_from(1, gz)
    even, odd = pairs_from(0, gy), pairs_from(1, gy)

    offsets, flips = jnp.swapaxes(offsets, 1, 2), jnp.swapaxes(flips, 1, 2)
    k_same, k_cross, k_even, k_odd = edges(kappa, offsets, flips)
    k_cross = lax.ppermute(k_cross, GZ, cross)
    k_same = lax.ppermute(k_same, GZ, same)
    k_even = lax.ppermute(k_even, "gy", even)
    k_odd = lax.ppermute(k_odd, "gy", odd)
    u, u_cross = update(coeffs, iterate, basis)
    u_out, u_same, u_even, u_odd, base, wz, wy = sketch(u, kappa, rhs, offsets, flips, k_same, k_cross, k_even, k_odd)
    got = lax.ppermute(u_same, GZ, same)
    value = u_same[ny : ny + 2] + got[ny : ny + 2]
    u_same = got
    terms = [value]
    for axis in ("gy", "x", "z"):
        for step in rounds(sizes[axis]) if sizes[axis] > 1 else ():
            value = sum(terms[1:], terms[0])
            if axis == "x":
                u_cross, value = lax.optimization_barrier((u_cross, value))
            terms = [value] + [lax.ppermute(value, axis, pairs) for pairs in step.values()]
    u_cross = lax.ppermute(u_cross, GZ, cross)
    u_even = lax.ppermute(u_even, "gy", even)
    u_odd = lax.ppermute(u_odd, "gy", odd)
    residual = with_halo(base, wz, wy, u_same, u_cross, u_even, u_odd)
    return u_out, residual, scaled(*terms).reshape(SK)


def build(mesh, outer):
    gy = mesh.shape["gy"]
    finer = Mesh(mesh.devices.reshape(*outer, gy), (*GZ, "gy"))
    sizes = dict(finer.shape)
    field = P(GZ, "gy", None)
    return jax.shard_map(
        functools.partial(shards, sizes),
        mesh=finer,
        in_specs=(field, P(None, GZ, "gy", None), P(), field, field, field, field),
        out_specs=(field, field, P()),
        check_vma=False,
    )


def solution(mesh):
    return build(mesh, (mesh.shape["gz"] // 8, 4, 2))
```

```python
import functools

import jax
import jax.numpy as jnp
from jax import lax
from jax.experimental import pallas as pl
from jax.experimental.pallas import tpu as pltpu
from jax.sharding import Mesh
from jax.sharding import PartitionSpec as P


SK = 2048
BLK = 128
ROWS = SK // BLK
GROUP = 4
GZ = ("z", "x", "core")
HBM = pl.BlockSpec(memory_space=pltpu.HBM)
VMEM = pl.BlockSpec(memory_space=pltpu.VMEM)


def f32(*shape):
    return jax.ShapeDtypeStruct(shape, jnp.float32)


def parities():
    return lax.axis_index("core") == 0, lax.rem(lax.axis_index("gy"), 2) == 0


def columns(table):
    return jnp.transpose(table)


def inside():
    z, x, core, y = (lax.axis_index(a) for a in (*GZ, "gy"))
    spot = (z * lax.axis_size("x") + x) * 2 + core
    last = lax.axis_size("z") * lax.axis_size("x") * 2 - 1
    outer = (spot == 0) | (spot == last), (y == 0) | (y == lax.axis_size("gy") - 1)
    return [jnp.where(edge, 0.0, 1.0) for edge in outer]


def edge_kernel(k_hbm, off_hbm, flip_hbm, same_ref, cross_ref, even_ref, odd_ref, k_ref, off_ref, flip_ref, sems):
    copies = [
        pltpu.make_async_copy(source, target, sems.at[i])
        for i, (source, target) in enumerate(((k_hbm, k_ref), (off_hbm, off_ref), (flip_hbm, flip_ref)))
    ]
    for copy in copies:
        copy.start()
    for copy in copies:
        copy.wait()
    nz, ny, nx = k_ref.shape
    blocks = nx // BLK
    core0, even = parities()

    def both(low, high):
        return jnp.where(core0, high, low), jnp.where(core0, low, high)

    same_ref[:ny], cross_ref[:ny] = both(k_ref[0], k_ref[1])
    offs = [off_ref[z].astype(jnp.float32) for z in range(nz)]
    signs = [(2 * flip_ref[z] - 1).astype(jnp.float32) for z in range(nz)]
    same_ref[ny:, :ny], cross_ref[ny:, :ny] = both(offs[0], offs[1])
    same_ref[ny:, BLK : BLK + ny], cross_ref[ny:, BLK : BLK + ny] = both(signs[0], signs[1])
    for z in range(nz):
        off_t, sign_t = columns(offs[z]), columns(signs[z])
        for q in range(blocks):
            lanes = slice(q * BLK, (q + 1) * BLK)
            for at, table in ((nz + z, off_t), (2 * nz + z, sign_t)):
                low = jnp.broadcast_to(table[:1, q : q + 1], (1, BLK))
                high = jnp.broadcast_to(table[ny - 1 :, q : q + 1], (1, BLK))
                even_ref[at : at + 1, lanes] = jnp.where(even, high, low)
                odd_ref[at : at + 1, lanes] = jnp.where(even, low, high)
        low, high = k_ref[z, :1, :], k_ref[z, ny - 1 :, :]
        even_ref[z : z + 1, :] = jnp.where(even, high, low)
        odd_ref[z : z + 1, :] = jnp.where(even, low, high)
    rest = slice(3 * nz, 8)
    even_ref[rest, :] = jnp.zeros((8 - 3 * nz, nx), jnp.float32)
    odd_ref[rest, :] = jnp.zeros((8 - 3 * nz, nx), jnp.float32)


def edges(kappa, offsets, flips):
    _, ny, nx = kappa.shape
    plane, line = f32(ny + 8, nx), f32(8, nx)
    return pl.pallas_call(
        edge_kernel,
        out_shape=(plane, plane, line, line),
        in_specs=[HBM] * 3,
        out_specs=(VMEM,) * 4,
        scratch_shapes=[pltpu.VMEM(v.shape, v.dtype) for v in (kappa, offsets, flips)] + [pltpu.SemaphoreType.DMA((3,))],
        compiler_params=pltpu.CompilerParams(vmem_limit_bytes=8 << 20),
        cost_estimate=pl.CostEstimate(flops=1 << 32, bytes_accessed=1 << 28, transcendentals=0),
        name="edges",
    )(*(pltpu.with_memory_space_constraint(v, pltpu.HBM) for v in (kappa, offsets, flips)))


def update_kernel(coeff_ref, iterate_ref, basis_ref, u_ref, uc_ref, splat):
    kb, nz, ny, nx = basis_ref.shape
    core0, _ = parities()
    rounded = coeff_ref[...].astype(jnp.bfloat16).astype(jnp.float32)
    for k in range(kb):
        splat[k] = jnp.broadcast_to(rounded[:, k : k + 1], (8, BLK))

    @pl.loop(0, ny // 16)
    def _(i):
        rows = pl.ds(pl.multiple_of(i * 16, 16), 16)

        @pl.loop(0, nx // (2 * BLK))
        def _(j):
            lanes = [pl.ds(pl.multiple_of((2 * j + h) * BLK, BLK), BLK) for h in range(2)]
            spots = [(z, rows, part) for z in range(nz) for part in lanes]
            acc = [iterate_ref[spot] for spot in spots]
            for k in range(kb):
                scale = jnp.concatenate([splat[k]] * 2, 0)
                for n, spot in enumerate(spots):
                    acc[n] = acc[n] + scale * basis_ref[(k, *spot)].astype(jnp.float32)
            for n, spot in enumerate(spots):
                u_ref[spot] = acc[n]
            for n, part in enumerate(lanes):
                uc_ref[rows, part] = jnp.where(core0, acc[n], acc[len(lanes) + n])


def update(coeffs, iterate, basis):
    kb = basis.shape[0]
    return pl.pallas_call(
        update_kernel,
        out_shape=(f32(*iterate.shape), f32(*iterate.shape[1:])),
        in_specs=[VMEM] * 3,
        out_specs=(VMEM, VMEM),
        scratch_shapes=[pltpu.VMEM((kb, 8, BLK), jnp.float32)],
        compiler_params=pltpu.CompilerParams(vmem_limit_bytes=16 << 20),
        cost_estimate=pl.CostEstimate(flops=1 << 24, bytes_accessed=2 * basis.size, transcendentals=0),
        name="update",
    )(coeffs.reshape(1, kb), iterate, basis)


def lane_gather(values, index):
    numbers = lax.GatherDimensionNumbers(
        offset_dims=(),
        collapsed_slice_dims=(1,),
        start_index_map=(1,),
        operand_batching_dims=(0,),
        start_indices_batching_dims=(0,),
    )
    return lax.gather(values, index[..., None], numbers, (1, 1), mode=lax.GatherScatterMode.PROMISE_IN_BOUNDS)


def sketch_kernel(
    u_ref, k_ref, rhs_ref, off_ref, flip_ref, same_ref, cross_ref, even_ref, odd_ref,
    out_ref, us_ref, ue_ref, uo_ref, base_ref, wz_ref, wy_ref,
    hz_ref, hy_ref, sem,
):
    nz, ny, nx = u_ref.shape
    core0, even = parities()
    has_cross, has_odd = inside()
    blocks = nx // BLK
    store = pltpu.make_async_copy(u_ref, out_ref, sem)
    store.start()

    for z in range(nz):
        low, high = u_ref[z, :1, :], u_ref[z, ny - 1 :, :]
        ue_ref[z : z + 1, :] = jnp.where(even, high, low)
        uo_ref[z : z + 1, :] = jnp.where(even, low, high)

    lane = lax.broadcasted_iota(jnp.int32, (8, BLK), 1)
    line = lax.broadcasted_iota(jnp.int32, (8, BLK), 0)
    odd_lines = odd_ref[...] * has_odd
    low_y = jnp.where(even, odd_lines, even_ref[...])
    high_y = jnp.where(even, even_ref[...], odd_lines)
    cells = [(z, q) for z in range(nz) for q in range(blocks)]

    def lanes(q):
        return slice(q * BLK, (q + 1) * BLK)

    def tile(ref, y):
        return {(z, q): ref[z, y : y + 8, lanes(q)] for z, q in cells}

    def up(tiles):
        return {c: pltpu.roll(t, 7, 0) for c, t in tiles.items()}

    u, k = tile(u_ref, 0), tile(k_ref, 0)
    u_up, k_up = up(u), up(k)
    below = None
    for y in range(0, ny, 8):
        rows = slice(y, y + 8)
        if y + 8 < ny:
            u_next, k_next = tile(u_ref, y + 8), tile(k_ref, y + 8)
            u_next_up, k_next_up = up(u_next), up(k_next)
        else:
            u_next = k_next = None
            u_next_up = {c: 0.0 for c in cells}
            k_next_up = {(z, q): high_y[z : z + 1, lanes(q)] for z, q in cells}
        between = {q: (k[0, q] + k[1, q]) * (u[0, q] - u[1, q]) for q in range(blocks)}
        above = {}
        for z in range(nz):
            swap = core0 if z else jnp.logical_not(core0)
            u_right = {q: pltpu.roll(u[z, q], BLK - 1, 1) for q in range(blocks)}
            k_right = {q: pltpu.roll(k[z, q], BLK - 1, 1) for q in range(blocks)}
            u_right[blocks] = k_right[blocks] = 0.0
            left = None
            for q in range(blocks):
                c = (z, q)
                pair = k[c] + jnp.where(swap, same_ref[rows, lanes(q)], cross_ref[rows, lanes(q)] * has_cross)
                wz = 0.5 * pair
                wz_ref[z, rows, lanes(q)] = wz
                hz_ref[z, rows, lanes(q)] = wz * u[c]
                total = pair * u[c]
                total = total - between[q] if z else total + between[q]
                flow = (k[c] + jnp.where(line == 7, k_next_up[c], k_up[c])) * (
                    u[c] - jnp.where(line == 7, u_next_up[c], u_up[c])
                )
                above[c] = pltpu.roll(flow, 1, 0)
                if y == 0:
                    edge = k[c] + low_y[z : z + 1, lanes(q)]
                    wy_ref[z : z + 1, lanes(q)] = 0.5 * edge[:1]
                    edge = edge * u[c]
                    hy_ref[z : z + 1, lanes(q)] = 0.5 * edge[:1]
                    before = -edge
                else:
                    before = below[c]
                if y == ny - 8:
                    edge = k[c] + high_y[z : z + 1, lanes(q)]
                    wy_ref[nz + z : nz + z + 1, lanes(q)] = 0.5 * edge[7:]
                    hy_ref[nz + z : nz + z + 1, lanes(q)] = 0.5 * (edge * u[c])[7:]
                total = total + (flow - jnp.where(line == 0, before, above[c]))
                flow = (k[c] + jnp.where(lane == BLK - 1, k_right[q + 1], k_right[q])) * (
                    u[c] - jnp.where(lane == BLK - 1, u_right[q + 1], u_right[q])
                )
                turned = pltpu.roll(flow, 1, 1)
                before = -k[c] * u[c] if q == 0 else left
                total = total + (flow - jnp.where(lane == 0, before, turned))
                left = turned
                base_ref[z, rows, lanes(q)] = (rhs_ref[z, rows, lanes(q)] - 0.05 * u[c]) - 0.5 * total
        below = above
        u, k, u_up, k_up = u_next, k_next, u_next_up, k_next_up

    for y in range(0, ny, 8):
        rows = slice(y, y + 8)
        us_ref[rows, :] = jnp.where(core0, u_ref[1, rows, :], u_ref[0, rows, :])

    sums = []
    block_of = jnp.right_shift(lax.broadcasted_iota(jnp.int32, (blocks, nx), 1), 7)
    widen = (block_of == lax.broadcasted_iota(jnp.int32, (blocks, nx), 0)).astype(jnp.float32).astype(jnp.bfloat16)

    def place(offs, signs):
        slot = lax.broadcasted_iota(jnp.int32, (ROWS, offs.shape[1]), 0)
        return jnp.where(slot == jnp.right_shift(offs, 7), signs, 0.0).astype(jnp.bfloat16)

    def turn(block, by):
        spot = lax.broadcasted_iota(jnp.int32, block.shape, 1)
        here = spot >= by
        block = lane_gather(block, (spot - by) & (BLK - 1))
        high = block.astype(jnp.bfloat16)
        low = (block - high.astype(jnp.float32)).astype(jnp.bfloat16)
        none = jnp.zeros_like(high)
        return [jnp.concatenate([jnp.where(here, t, none), jnp.where(here, none, t)], 1) for t in (high, low)]

    def add(spots, terms):
        at = jnp.concatenate(spots * 2, 1)
        values = jnp.concatenate([t[0] for t in terms] + [t[1] for t in terms], 0)
        sums.append(jnp.dot(at, values, preferred_element_type=jnp.float32))

    for z in range(nz):
        swap = core0 if z else jnp.logical_not(core0)
        theirs = jnp.where(swap, same_ref[ny:, : 2 * BLK], cross_ref[ny:, : 2 * BLK] * has_cross)
        mine = (2 * flip_ref[z] - 1).astype(jnp.float32)
        for source, offs, signs in (
            (base_ref, off_ref[z], mine),
            (hz_ref, theirs[:, :ny].astype(jnp.int32), theirs[:, BLK : BLK + ny]),
        ):
            turned = columns((offs & (BLK - 1)).astype(jnp.float32)).astype(jnp.bfloat16)
            turned = jnp.dot(turned, widen, preferred_element_type=jnp.float32).astype(jnp.int32)
            for start in range(0, blocks, GROUP):
                group = range(start, start + GROUP)
                at = place(
                    jnp.concatenate([offs[q : q + 1, :] for q in group], 1),
                    jnp.concatenate([signs[q : q + 1, :] for q in group], 1),
                )
                add([at], [turn(source[z, :, lanes(q)], turned[:, lanes(q)]) for q in group])

    hy_ref[2 * nz :, :] = jnp.zeros((16 - 2 * nz, nx), jnp.float32)
    unused = jnp.zeros((16 - 2 * nz, nx), jnp.float32)
    y_offs = jnp.concatenate([low_y[nz : 2 * nz], high_y[nz : 2 * nz], unused], 0).astype(jnp.int32)
    y_signs = jnp.concatenate([low_y[2 * nz : 3 * nz], high_y[2 * nz : 3 * nz], unused], 0)
    spots, terms = [], []
    for q in range(blocks):
        offs, signs = y_offs[:, lanes(q)], y_signs[:, lanes(q)]
        spots.append(place(jnp.transpose(offs[:, :1]), jnp.transpose(signs[:, :1])))
        terms.append(turn(hy_ref[:, lanes(q)], offs & (BLK - 1)))
    add(spots, terms)

    got = sum(sums[1:], sums[0])
    carry = got[:, BLK:]
    part = got[:, :BLK] + jnp.concatenate([carry[ROWS - 1 :], carry[: ROWS - 1]], 0)
    us_ref[ny:, :] = jnp.zeros((8, nx), jnp.float32)
    for m in range(ROWS):
        at = ny + m // blocks
        us_ref[at : at + 1, lanes(m % blocks)] = part[m : m + 1]
    store.wait()


def sketch(u, *rest):
    nz, ny, nx = u.shape
    field = f32(nz, ny, nx)
    return pl.pallas_call(
        sketch_kernel,
        out_shape=(field, f32(ny + 8, nx), f32(nz, nx), f32(nz, nx), field, field, f32(2 * nz, nx)),
        in_specs=[VMEM] * 9,
        out_specs=(pl.BlockSpec(memory_space=pl.ANY),) + (VMEM,) * 6,
        scratch_shapes=[
            pltpu.VMEM((nz, ny, nx), jnp.float32),
            pltpu.VMEM((16, nx), jnp.float32),
            pltpu.SemaphoreType.DMA,
        ],
        compiler_params=pltpu.CompilerParams(vmem_limit_bytes=16 << 20),
        cost_estimate=pl.CostEstimate(flops=1 << 24, bytes_accessed=16 << 20, transcendentals=0),
        name="sketch",
    )(u, *rest)


def halo_kernel(base_ref, wz_ref, wy_ref, us_ref, uc_ref, ue_ref, uo_ref, res_ref):
    nz, ny, _ = base_ref.shape
    core0, even = parities()
    has_cross, has_odd = inside()
    odd_lines = uo_ref[...] * has_odd
    low_y = jnp.where(even, odd_lines, ue_ref[...])
    high_y = jnp.where(even, ue_ref[...], odd_lines)
    for z in range(nz):
        swap = core0 if z else jnp.logical_not(core0)
        for y in range(0, ny, 8):
            rows = slice(y, y + 8)
            value = base_ref[z, rows, :] + wz_ref[z, rows, :] * jnp.where(
                swap, us_ref[rows, :], uc_ref[rows, :] * has_cross
            )
            res_ref[z, rows, :] = value
        res_ref[z, :1, :] += wy_ref[z : z + 1, :] * low_y[z : z + 1, :]
        res_ref[z, ny - 1 :, :] += wy_ref[nz + z : nz + z + 1, :] * high_y[z : z + 1, :]


def with_halo(base, *rest):
    return pl.pallas_call(
        halo_kernel,
        out_shape=f32(*base.shape),
        in_specs=[VMEM] * 7,
        out_specs=VMEM,
        compiler_params=pltpu.CompilerParams(vmem_limit_bytes=8 << 20),
        cost_estimate=pl.CostEstimate(flops=1 << 20, bytes_accessed=2 << 20, transcendentals=0),
        name="halo",
    )(base, *rest)


def scale_kernel(*refs):
    sketch = refs[0][...]
    for ref in refs[1:-1]:
        sketch = sketch + ref[...]
    mean = jnp.sum(sketch * sketch) * (1.0 / SK)
    unit = sketch / jnp.sqrt(jnp.broadcast_to(mean + 1e-06, sketch.shape))
    wide = sketch.shape[1] // BLK
    for m in range(ROWS):
        refs[-1][m : m + 1, :] = unit[m // wide : m // wide + 1, m % wide * BLK : (m % wide + 1) * BLK]


def scaled(*parts):
    return pl.pallas_call(
        scale_kernel,
        out_shape=f32(ROWS, BLK),
        in_specs=[VMEM] * len(parts),
        out_specs=VMEM,
        compiler_params=pltpu.CompilerParams(vmem_limit_bytes=4 << 20),
        name="scaled",
    )(*parts)


def both_ways(pairs):
    return pairs + [(b, a) for a, b in pairs]


def pairs_from(first, count):
    return both_ways([(i, i + 1) for i in range(first, count - 1, 2)])


def rounds(count):
    pairs = {"pair": pairs_from(0, count)}
    if count == 2:
        return [pairs]
    if count == 4:
        return [{f"apart{k}": [(i, i ^ k) for i in range(4)] for k in (3, 2, 1)}]
    third = both_ways([(0, 5), (1, 4), (2, 7), (3, 6)])
    second = [(i, (i - 2) % 8) for i in range(0, 8, 2)] + [(i, (i + 2) % 8) for i in range(1, 8, 2)]
    first = both_ways([(i, (i + 1) % 8) for i in range(1, 8, 2)])
    return [pairs, {"apart3": third, "apart2": second, "apart1": first}]


def shards(sizes, *arrays):
    return cycle_end(sizes, *arrays)


def cycle_end(sizes, iterate, basis, coeffs, rhs, kappa, offsets, flips):
    gz = sizes["z"] * sizes["x"] * sizes["core"]
    gy = sizes["gy"]
    _, ny, _ = kappa.shape
    same, cross = pairs_from(0, gz), pairs_from(1, gz) + [(0, 0), (gz - 1, gz - 1)]
    even, odd = pairs_from(0, gy), pairs_from(1, gy) + [(0, 0), (gy - 1, gy - 1)]

    offsets, flips = jnp.swapaxes(offsets, 1, 2), jnp.swapaxes(flips, 1, 2)
    k_same, k_cross, k_even, k_odd = edges(kappa, offsets, flips)
    k_cross = lax.ppermute(k_cross, GZ, cross)
    k_same = lax.ppermute(k_same, GZ, same)
    k_even = lax.ppermute(k_even, "gy", even)
    k_odd = lax.ppermute(k_odd, "gy", odd)
    u, u_cross = update(coeffs, iterate, basis)
    u_out, u_same, u_even, u_odd, base, wz, wy = sketch(u, kappa, rhs, offsets, flips, k_same, k_cross, k_even, k_odd)
    got = lax.ppermute(u_same, GZ, same)
    value = u_same[ny : ny + 2] + got[ny : ny + 2]
    u_same = got
    terms = [value]
    for axis in ("gy", "x", "z"):
        for step in rounds(sizes[axis]) if sizes[axis] > 1 else ():
            value = sum(terms[1:], terms[0])
            if axis == "x":
                u_cross, value = lax.optimization_barrier((u_cross, value))
            terms = [value] + [lax.ppermute(value, axis, pairs) for pairs in step.values()]
    u_cross = lax.ppermute(u_cross, GZ, cross)
    u_even = lax.ppermute(u_even, "gy", even)
    u_odd = lax.ppermute(u_odd, "gy", odd)
    residual = with_halo(base, wz, wy, u_same, u_cross, u_even, u_odd)
    return u_out, residual, scaled(*terms).reshape(SK)


def build(mesh, outer):
    gy = mesh.shape["gy"]
    finer = Mesh(mesh.devices.reshape(*outer, gy), (*GZ, "gy"))
    sizes = dict(finer.shape)
    field = P(GZ, "gy", None)
    return jax.shard_map(
        functools.partial(shards, sizes),
        mesh=finer,
        in_specs=(field, P(None, GZ, "gy", None), P(), field, field, field, field),
        out_specs=(field, field, P()),
        check_vma=False,
    )


def solution(mesh):
    return build(mesh, (mesh.shape["gz"] // 8, 4, 2))
```

```python
import functools

import jax
import jax.numpy as jnp
from jax import lax
from jax.experimental import pallas as pl
from jax.experimental.pallas import tpu as pltpu
from jax.sharding import Mesh
from jax.sharding import PartitionSpec as P


SK = 2048
BLK = 128
ROWS = SK // BLK
GROUP = 4
GZ = ("z", "x", "core")
HBM = pl.BlockSpec(memory_space=pltpu.HBM)
VMEM = pl.BlockSpec(memory_space=pltpu.VMEM)


def f32(*shape):
    return jax.ShapeDtypeStruct(shape, jnp.float32)


def parities():
    return lax.axis_index("core") == 0, lax.rem(lax.axis_index("gy"), 2) == 0


def columns(table):
    return jnp.transpose(table)


def inside():
    z, x, core, y = (lax.axis_index(a) for a in (*GZ, "gy"))
    spot = (z * lax.axis_size("x") + x) * 2 + core
    last = lax.axis_size("z") * lax.axis_size("x") * 2 - 1
    outer = (spot == 0) | (spot == last), (y == 0) | (y == lax.axis_size("gy") - 1)
    return [jnp.where(edge, 0.0, 1.0) for edge in outer]


def edge_kernel(k_hbm, off_hbm, flip_hbm, same_ref, cross_ref, even_ref, odd_ref, k_ref, off_ref, flip_ref, sems):
    copies = [
        pltpu.make_async_copy(source, target, sems.at[i])
        for i, (source, target) in enumerate(((k_hbm, k_ref), (off_hbm, off_ref), (flip_hbm, flip_ref)))
    ]
    for copy in copies:
        copy.start()
    for copy in copies:
        copy.wait()
    nz, ny, nx = k_ref.shape
    blocks = nx // BLK
    core0, even = parities()

    def both(low, high):
        return jnp.where(core0, high, low), jnp.where(core0, low, high)

    same_ref[:ny], cross_ref[:ny] = both(k_ref[0], k_ref[1])
    offs = [off_ref[z].astype(jnp.float32) for z in range(nz)]
    signs = [(2 * flip_ref[z] - 1).astype(jnp.float32) for z in range(nz)]
    same_ref[ny:, :ny], cross_ref[ny:, :ny] = both(offs[0], offs[1])
    same_ref[ny:, BLK : BLK + ny], cross_ref[ny:, BLK : BLK + ny] = both(signs[0], signs[1])
    for z in range(nz):
        off_t, sign_t = columns(offs[z]), columns(signs[z])
        for q in range(blocks):
            lanes = slice(q * BLK, (q + 1) * BLK)
            for at, table in ((nz + z, off_t), (2 * nz + z, sign_t)):
                low = jnp.broadcast_to(table[:1, q : q + 1], (1, BLK))
                high = jnp.broadcast_to(table[ny - 1 :, q : q + 1], (1, BLK))
                even_ref[at : at + 1, lanes] = jnp.where(even, high, low)
                odd_ref[at : at + 1, lanes] = jnp.where(even, low, high)
        low, high = k_ref[z, :1, :], k_ref[z, ny - 1 :, :]
        even_ref[z : z + 1, :] = jnp.where(even, high, low)
        odd_ref[z : z + 1, :] = jnp.where(even, low, high)
    rest = slice(3 * nz, 8)
    even_ref[rest, :] = jnp.zeros((8 - 3 * nz, nx), jnp.float32)
    odd_ref[rest, :] = jnp.zeros((8 - 3 * nz, nx), jnp.float32)


def edges(kappa, offsets, flips):
    _, ny, nx = kappa.shape
    plane, line = f32(ny + 8, nx), f32(8, nx)
    return pl.pallas_call(
        edge_kernel,
        out_shape=(plane, plane, line, line),
        in_specs=[HBM] * 3,
        out_specs=(VMEM,) * 4,
        scratch_shapes=[pltpu.VMEM(v.shape, v.dtype) for v in (kappa, offsets, flips)] + [pltpu.SemaphoreType.DMA((3,))],
        compiler_params=pltpu.CompilerParams(vmem_limit_bytes=8 << 20),
        cost_estimate=pl.CostEstimate(flops=1 << 32, bytes_accessed=1 << 28, transcendentals=0),
        name="edges",
    )(*(pltpu.with_memory_space_constraint(v, pltpu.HBM) for v in (kappa, offsets, flips)))


def update_kernel(coeff_ref, iterate_ref, basis_ref, u_ref, us_ref, uc_ref, splat):
    kb, nz, ny, _ = basis_ref.shape
    core0, _ = parities()
    rounded = coeff_ref[...].astype(jnp.bfloat16).astype(jnp.float32)
    for k in range(kb):
        splat[k] = jnp.broadcast_to(rounded[:, k : k + 1], (8, BLK))

    @pl.loop(0, ny // 32)
    def _(i):
        rows = [pl.ds(pl.multiple_of(i * 32 + 16 * h, 16), 16) for h in range(2)]
        spots = [(z, part, slice(None)) for z in range(nz) for part in rows]
        acc = [iterate_ref[spot] for spot in spots]
        for k in range(kb):
            scale = jnp.concatenate([splat[k]] * 2, 0)
            for n, spot in enumerate(spots):
                acc[n] = acc[n] + scale * basis_ref[(k, *spot)].astype(jnp.float32)
        for n, spot in enumerate(spots):
            u_ref[spot] = acc[n]
        for n, part in enumerate(rows):
            us_ref[part] = jnp.where(core0, acc[len(rows) + n], acc[n])
            uc_ref[part] = jnp.where(core0, acc[n], acc[len(rows) + n])


def tiled(value):
    *lead, ny, nx = value.shape
    value = jnp.swapaxes(value.reshape(*lead, ny // 8, 8, nx // BLK, BLK), -3, -2)
    return value.reshape(*lead, ny * nx // BLK, BLK)


def untiled(value, nx):
    *lead, rows, _ = value.shape
    value = jnp.swapaxes(value.reshape(*lead, rows * BLK // (8 * nx), nx // BLK, 8, BLK), -3, -2)
    return value.reshape(*lead, rows * BLK // nx, nx)


def update(coeffs, iterate, basis):
    kb, nx = basis.shape[0], basis.shape[3]
    iterate, basis = tiled(iterate), tiled(basis)
    values = pl.pallas_call(
        update_kernel,
        out_shape=(f32(*iterate.shape), f32(*iterate.shape[1:]), f32(*iterate.shape[1:])),
        in_specs=[VMEM] * 3,
        out_specs=(VMEM,) * 3,
        scratch_shapes=[pltpu.VMEM((kb, 8, BLK), jnp.float32)],
        compiler_params=pltpu.CompilerParams(vmem_limit_bytes=16 << 20),
        cost_estimate=pl.CostEstimate(flops=1 << 24, bytes_accessed=2 * basis.size, transcendentals=0),
        name="update",
    )(coeffs.reshape(1, kb), iterate, basis)
    return [untiled(value, nx) for value in values]


def lane_gather(values, index):
    numbers = lax.GatherDimensionNumbers(
        offset_dims=(),
        collapsed_slice_dims=(1,),
        start_index_map=(1,),
        operand_batching_dims=(0,),
        start_indices_batching_dims=(0,),
    )
    return lax.gather(values, index[..., None], numbers, (1, 1), mode=lax.GatherScatterMode.PROMISE_IN_BOUNDS)


def sketch_kernel(
    u_ref, k_ref, rhs_ref, off_ref, flip_ref, same_ref, cross_ref, even_ref, odd_ref,
    out_ref, ue_ref, uo_ref, base_ref, wz_ref, wy_ref, part_ref,
    hz_ref, hy_ref, sem,
):
    nz, ny, nx = u_ref.shape
    core0, even = parities()
    has_cross, has_odd = inside()
    blocks = nx // BLK
    store = pltpu.make_async_copy(u_ref, out_ref, sem)
    store.start()

    for z in range(nz):
        low, high = u_ref[z, :1, :], u_ref[z, ny - 1 :, :]
        ue_ref[z : z + 1, :] = jnp.where(even, high, low)
        uo_ref[z : z + 1, :] = jnp.where(even, low, high)

    lane = lax.broadcasted_iota(jnp.int32, (8, BLK), 1)
    line = lax.broadcasted_iota(jnp.int32, (8, BLK), 0)
    odd_lines = odd_ref[...] * has_odd
    low_y = jnp.where(even, odd_lines, even_ref[...])
    high_y = jnp.where(even, even_ref[...], odd_lines)
    cells = [(z, q) for z in range(nz) for q in range(blocks)]

    def lanes(q):
        return slice(q * BLK, (q + 1) * BLK)

    def tile(ref, y):
        return {(z, q): ref[z, y : y + 8, lanes(q)] for z, q in cells}

    def up(tiles):
        return {c: pltpu.roll(t, 7, 0) for c, t in tiles.items()}

    u, k = tile(u_ref, 0), tile(k_ref, 0)
    u_up, k_up = up(u), up(k)
    below = None
    for y in range(0, ny, 8):
        rows = slice(y, y + 8)
        if y + 8 < ny:
            u_next, k_next = tile(u_ref, y + 8), tile(k_ref, y + 8)
            u_next_up, k_next_up = up(u_next), up(k_next)
        else:
            u_next = k_next = None
            u_next_up = {c: 0.0 for c in cells}
            k_next_up = {(z, q): high_y[z : z + 1, lanes(q)] for z, q in cells}
        between = {q: (k[0, q] + k[1, q]) * (u[0, q] - u[1, q]) for q in range(blocks)}
        above = {}
        for z in range(nz):
            swap = core0 if z else jnp.logical_not(core0)
            u_right = {q: pltpu.roll(u[z, q], BLK - 1, 1) for q in range(blocks)}
            k_right = {q: pltpu.roll(k[z, q], BLK - 1, 1) for q in range(blocks)}
            u_right[blocks] = k_right[blocks] = 0.0
            left = None
            for q in range(blocks):
                c = (z, q)
                pair = k[c] + jnp.where(swap, same_ref[rows, lanes(q)], cross_ref[rows, lanes(q)] * has_cross)
                wz = 0.5 * pair
                wz_ref[z, rows, lanes(q)] = wz
                hz_ref[z, rows, lanes(q)] = wz * u[c]
                total = pair * u[c]
                total = total - between[q] if z else total + between[q]
                flow = (k[c] + jnp.where(line == 7, k_next_up[c], k_up[c])) * (
                    u[c] - jnp.where(line == 7, u_next_up[c], u_up[c])
                )
                above[c] = pltpu.roll(flow, 1, 0)
                if y == 0:
                    edge = k[c] + low_y[z : z + 1, lanes(q)]
                    wy_ref[z : z + 1, lanes(q)] = 0.5 * edge[:1]
                    edge = edge * u[c]
                    hy_ref[z : z + 1, lanes(q)] = 0.5 * edge[:1]
                    before = -edge
                else:
                    before = below[c]
                if y == ny - 8:
                    edge = k[c] + high_y[z : z + 1, lanes(q)]
                    wy_ref[nz + z : nz + z + 1, lanes(q)] = 0.5 * edge[7:]
                    hy_ref[nz + z : nz + z + 1, lanes(q)] = 0.5 * (edge * u[c])[7:]
                total = total + (flow - jnp.where(line == 0, before, above[c]))
                flow = (k[c] + jnp.where(lane == BLK - 1, k_right[q + 1], k_right[q])) * (
                    u[c] - jnp.where(lane == BLK - 1, u_right[q + 1], u_right[q])
                )
                turned = pltpu.roll(flow, 1, 1)
                before = -k[c] * u[c] if q == 0 else left
                total = total + (flow - jnp.where(lane == 0, before, turned))
                left = turned
                base_ref[z, rows, lanes(q)] = (rhs_ref[z, rows, lanes(q)] - 0.05 * u[c]) - 0.5 * total
        below = above
        u, k, u_up, k_up = u_next, k_next, u_next_up, k_next_up

    sums = []
    block_of = jnp.right_shift(lax.broadcasted_iota(jnp.int32, (blocks, nx), 1), 7)
    widen = (block_of == lax.broadcasted_iota(jnp.int32, (blocks, nx), 0)).astype(jnp.float32).astype(jnp.bfloat16)

    def place(offs, signs):
        slot = lax.broadcasted_iota(jnp.int32, (ROWS, offs.shape[1]), 0)
        return jnp.where(slot == jnp.right_shift(offs, 7), signs, 0.0).astype(jnp.bfloat16)

    def turn(block, by):
        spot = lax.broadcasted_iota(jnp.int32, block.shape, 1)
        here = spot >= by
        block = lane_gather(block, (spot - by) & (BLK - 1))
        high = block.astype(jnp.bfloat16)
        low = (block - high.astype(jnp.float32)).astype(jnp.bfloat16)
        none = jnp.zeros_like(high)
        return [jnp.concatenate([jnp.where(here, t, none), jnp.where(here, none, t)], 1) for t in (high, low)]

    def add(spots, terms):
        at = jnp.concatenate(spots * 2, 1)
        values = jnp.concatenate([t[0] for t in terms] + [t[1] for t in terms], 0)
        sums.append(jnp.dot(at, values, preferred_element_type=jnp.float32))

    for z in range(nz):
        swap = core0 if z else jnp.logical_not(core0)
        theirs = jnp.where(swap, same_ref[ny:, : 2 * BLK], cross_ref[ny:, : 2 * BLK] * has_cross)
        mine = (2 * flip_ref[z] - 1).astype(jnp.float32)
        for source, offs, signs in (
            (base_ref, off_ref[z], mine),
            (hz_ref, theirs[:, :ny].astype(jnp.int32), theirs[:, BLK : BLK + ny]),
        ):
            turned = columns((offs & (BLK - 1)).astype(jnp.float32)).astype(jnp.bfloat16)
            turned = jnp.dot(turned, widen, preferred_element_type=jnp.float32).astype(jnp.int32)
            for start in range(0, blocks, GROUP):
                group = range(start, start + GROUP)
                at = place(
                    jnp.concatenate([offs[q : q + 1, :] for q in group], 1),
                    jnp.concatenate([signs[q : q + 1, :] for q in group], 1),
                )
                add([at], [turn(source[z, :, lanes(q)], turned[:, lanes(q)]) for q in group])

    hy_ref[2 * nz :, :] = jnp.zeros((16 - 2 * nz, nx), jnp.float32)
    unused = jnp.zeros((16 - 2 * nz, nx), jnp.float32)
    y_offs = jnp.concatenate([low_y[nz : 2 * nz], high_y[nz : 2 * nz], unused], 0).astype(jnp.int32)
    y_signs = jnp.concatenate([low_y[2 * nz : 3 * nz], high_y[2 * nz : 3 * nz], unused], 0)
    spots, terms = [], []
    for q in range(blocks):
        offs, signs = y_offs[:, lanes(q)], y_signs[:, lanes(q)]
        spots.append(place(jnp.transpose(offs[:, :1]), jnp.transpose(signs[:, :1])))
        terms.append(turn(hy_ref[:, lanes(q)], offs & (BLK - 1)))
    add(spots, terms)

    got = sum(sums[1:], sums[0])
    carry = got[:, BLK:]
    part = got[:, :BLK] + jnp.concatenate([carry[ROWS - 1 :], carry[: ROWS - 1]], 0)
    for m in range(ROWS):
        part_ref[m // blocks : m // blocks + 1, lanes(m % blocks)] = part[m : m + 1]
    store.wait()


def sketch(u, *rest):
    nz, ny, nx = u.shape
    field = f32(nz, ny, nx)
    return pl.pallas_call(
        sketch_kernel,
        out_shape=(
            field, f32(nz, nx), f32(nz, nx), field, field, f32(2 * nz, nx), f32(SK // nx, nx),
        ),
        in_specs=[VMEM] * 9,
        out_specs=(pl.BlockSpec(memory_space=pl.ANY),) + (VMEM,) * 6,
        scratch_shapes=[
            pltpu.VMEM((nz, ny, nx), jnp.float32),
            pltpu.VMEM((16, nx), jnp.float32),
            pltpu.SemaphoreType.DMA,
        ],
        compiler_params=pltpu.CompilerParams(vmem_limit_bytes=16 << 20),
        cost_estimate=pl.CostEstimate(flops=1 << 24, bytes_accessed=16 << 20, transcendentals=0),
        name="sketch",
    )(u, *rest)


def halo_kernel(base_ref, wz_ref, wy_ref, us_ref, uc_ref, ue_ref, uo_ref, res_ref):
    nz, ny, _ = base_ref.shape
    core0, even = parities()
    has_cross, has_odd = inside()
    odd_lines = uo_ref[...] * has_odd
    low_y = jnp.where(even, odd_lines, ue_ref[...])
    high_y = jnp.where(even, ue_ref[...], odd_lines)
    for z in range(nz):
        swap = core0 if z else jnp.logical_not(core0)
        for y in range(0, ny, 8):
            rows = slice(y, y + 8)
            value = base_ref[z, rows, :] + wz_ref[z, rows, :] * jnp.where(
                swap, us_ref[rows, :], uc_ref[rows, :] * has_cross
            )
            res_ref[z, rows, :] = value
        res_ref[z, :1, :] += wy_ref[z : z + 1, :] * low_y[z : z + 1, :]
        res_ref[z, ny - 1 :, :] += wy_ref[nz + z : nz + z + 1, :] * high_y[z : z + 1, :]


def with_halo(base, *rest):
    return pl.pallas_call(
        halo_kernel,
        out_shape=f32(*base.shape),
        in_specs=[VMEM] * 7,
        out_specs=VMEM,
        compiler_params=pltpu.CompilerParams(vmem_limit_bytes=8 << 20),
        cost_estimate=pl.CostEstimate(flops=1 << 20, bytes_accessed=2 << 20, transcendentals=0),
        name="halo",
    )(base, *rest)


def scale_kernel(*refs):
    sketch = refs[0][...]
    for ref in refs[1:-1]:
        sketch = sketch + ref[...]
    mean = jnp.sum(sketch * sketch) * (1.0 / SK)
    unit = sketch / jnp.sqrt(jnp.broadcast_to(mean + 1e-06, sketch.shape))
    wide = sketch.shape[1] // BLK
    for m in range(ROWS):
        refs[-1][m : m + 1, :] = unit[m // wide : m // wide + 1, m % wide * BLK : (m % wide + 1) * BLK]


def scaled(*parts):
    return pl.pallas_call(
        scale_kernel,
        out_shape=f32(ROWS, BLK),
        in_specs=[VMEM] * len(parts),
        out_specs=VMEM,
        compiler_params=pltpu.CompilerParams(vmem_limit_bytes=4 << 20),
        name="scaled",
    )(*parts)


def both_ways(pairs):
    return pairs + [(b, a) for a, b in pairs]


def pairs_from(first, count):
    return both_ways([(i, i + 1) for i in range(first, count - 1, 2)])


def rounds(count):
    pairs = {"pair": pairs_from(0, count)}
    if count == 2:
        return [pairs]
    if count == 4:
        return [{f"apart{k}": [(i, i ^ k) for i in range(4)] for k in (3, 2, 1)}]
    third = both_ways([(0, 5), (1, 4), (2, 7), (3, 6)])
    second = [(i, (i - 2) % 8) for i in range(0, 8, 2)] + [(i, (i + 2) % 8) for i in range(1, 8, 2)]
    first = both_ways([(i, (i + 1) % 8) for i in range(1, 8, 2)])
    return [pairs, {"apart3": third, "apart2": second, "apart1": first}]


def shards(sizes, *arrays):
    return cycle_end(sizes, *arrays)


def cycle_end(sizes, iterate, basis, coeffs, rhs, kappa, offsets, flips):
    gz = sizes["z"] * sizes["x"] * sizes["core"]
    gy = sizes["gy"]
    same, cross = pairs_from(0, gz), pairs_from(1, gz) + [(0, 0), (gz - 1, gz - 1)]
    even, odd = pairs_from(0, gy), pairs_from(1, gy) + [(0, 0), (gy - 1, gy - 1)]

    offsets, flips = jnp.swapaxes(offsets, 1, 2), jnp.swapaxes(flips, 1, 2)
    k_same, k_cross, k_even, k_odd = edges(kappa, offsets, flips)
    k_cross = lax.ppermute(k_cross, GZ, cross)
    k_same = lax.ppermute(k_same, GZ, same)
    k_even = lax.ppermute(k_even, "gy", even)
    k_odd = lax.ppermute(k_odd, "gy", odd)
    u, u_same, u_cross = update(coeffs, iterate, basis)
    u_out, u_even, u_odd, base, wz, wy, part = sketch(
        u, kappa, rhs, offsets, flips, k_same, k_cross, k_even, k_odd
    )
    u_same, part = lax.optimization_barrier((u_same, part))
    value = part + lax.ppermute(part, GZ, same)
    terms = [value]
    for axis in ("gy", "x", "z"):
        for step in rounds(sizes[axis]) if sizes[axis] > 1 else ():
            value = sum(terms[1:], terms[0])
            if axis == "x":
                u_cross, value = lax.optimization_barrier((u_cross, value))
            terms = [value] + [lax.ppermute(value, axis, pairs) for pairs in step.values()]
    u_cross = lax.ppermute(u_cross, GZ, cross)
    u_same = lax.ppermute(u_same, GZ, same)
    u_even = lax.ppermute(u_even, "gy", even)
    u_odd = lax.ppermute(u_odd, "gy", odd)
    residual = with_halo(base, wz, wy, u_same, u_cross, u_even, u_odd)
    return u_out, residual, scaled(*terms).reshape(SK)


def build(mesh, outer):
    gy = mesh.shape["gy"]
    finer = Mesh(mesh.devices.reshape(*outer, gy), (*GZ, "gy"))
    sizes = dict(finer.shape)
    field = P(GZ, "gy", None)
    return jax.shard_map(
        functools.partial(shards, sizes),
        mesh=finer,
        in_specs=(field, P(None, GZ, "gy", None), P(), field, field, field, field),
        out_specs=(field, field, P()),
        check_vma=False,
    )


def solution(mesh):
    return build(mesh, (mesh.shape["gz"] // 8, 4, 2))
```

```python
import functools

import jax
import jax.numpy as jnp
from jax import lax
from jax.experimental import pallas as pl
from jax.experimental.pallas import tpu as pltpu
from jax.sharding import Mesh
from jax.sharding import PartitionSpec as P


SK = 2048
BLK = 128
ROWS = SK // BLK
GROUP = 4
GZ = ("z", "x", "core")
HBM = pl.BlockSpec(memory_space=pltpu.HBM)
VMEM = pl.BlockSpec(memory_space=pltpu.VMEM)


def f32(*shape):
    return jax.ShapeDtypeStruct(shape, jnp.float32)


def parities():
    return lax.axis_index("core") == 0, lax.rem(lax.axis_index("gy"), 2) == 0


def columns(table):
    return jnp.transpose(table)


def inside():
    z, x, core, y = (lax.axis_index(a) for a in (*GZ, "gy"))
    spot = (z * lax.axis_size("x") + x) * 2 + core
    last = lax.axis_size("z") * lax.axis_size("x") * 2 - 1
    outer = (spot == 0) | (spot == last), (y == 0) | (y == lax.axis_size("gy") - 1)
    return [jnp.where(edge, 0.0, 1.0) for edge in outer]


def edge_kernel(
    k_hbm, off_hbm, flip_hbm, same_ref, cross_ref, even_ref, odd_ref, low_ref, high_ref, off_ref, flip_ref, sems
):
    nz, ny, nx = k_hbm.shape
    core = lax.axis_index("core")
    moves = (
        (off_hbm, off_ref),
        (flip_hbm, flip_ref),
        (k_hbm.at[:, pl.ds(0, 8), :], low_ref),
        (k_hbm.at[:, pl.ds(ny - 8, 8), :], high_ref),
        (k_hbm.at[core], cross_ref.at[pl.ds(0, ny), :]),
        (k_hbm.at[1 - core], same_ref.at[pl.ds(0, ny), :]),
    )
    copies = [pltpu.make_async_copy(source, target, sems.at[i]) for i, (source, target) in enumerate(moves)]
    for copy in copies:
        copy.start()
    for copy in copies[:4]:
        copy.wait()
    blocks = nx // BLK
    core0, even = parities()

    def both(low, high):
        return jnp.where(core0, high, low), jnp.where(core0, low, high)

    offs = [off_ref[z].astype(jnp.float32) for z in range(nz)]
    signs = [(2 * flip_ref[z] - 1).astype(jnp.float32) for z in range(nz)]
    same_ref[ny:, :ny], cross_ref[ny:, :ny] = both(offs[0], offs[1])
    same_ref[ny:, BLK : BLK + ny], cross_ref[ny:, BLK : BLK + ny] = both(signs[0], signs[1])
    for z in range(nz):
        off_t, sign_t = columns(offs[z]), columns(signs[z])
        for q in range(blocks):
            lanes = slice(q * BLK, (q + 1) * BLK)
            for at, table in ((nz + z, off_t), (2 * nz + z, sign_t)):
                low = jnp.broadcast_to(table[:1, q : q + 1], (1, BLK))
                high = jnp.broadcast_to(table[ny - 1 :, q : q + 1], (1, BLK))
                even_ref[at : at + 1, lanes] = jnp.where(even, high, low)
                odd_ref[at : at + 1, lanes] = jnp.where(even, low, high)
        low, high = low_ref[z, :1, :], high_ref[z, 7:, :]
        even_ref[z : z + 1, :] = jnp.where(even, high, low)
        odd_ref[z : z + 1, :] = jnp.where(even, low, high)
    rest = slice(3 * nz, 8)
    even_ref[rest, :] = jnp.zeros((8 - 3 * nz, nx), jnp.float32)
    odd_ref[rest, :] = jnp.zeros((8 - 3 * nz, nx), jnp.float32)
    for copy in copies[4:]:
        copy.wait()


def edges(kappa, offsets, flips):
    nz, ny, nx = kappa.shape
    plane, line = f32(ny + 8, nx), f32(8, nx)
    return pl.pallas_call(
        edge_kernel,
        out_shape=(plane, plane, line, line),
        in_specs=[HBM] * 3,
        out_specs=(VMEM,) * 4,
        scratch_shapes=[pltpu.VMEM((nz, 8, nx), jnp.float32)] * 2
        + [pltpu.VMEM(v.shape, v.dtype) for v in (offsets, flips)]
        + [pltpu.SemaphoreType.DMA((6,))],
        compiler_params=pltpu.CompilerParams(vmem_limit_bytes=8 << 20),
        cost_estimate=pl.CostEstimate(flops=1 << 32, bytes_accessed=1 << 28, transcendentals=0),
        name="edges",
    )(*(pltpu.with_memory_space_constraint(v, pltpu.HBM) for v in (kappa, offsets, flips)))


def update_kernel(coeff_ref, iterate_ref, basis_ref, u_ref, us_ref, uc_ref, splat):
    kb, nz, ny, _ = basis_ref.shape
    core0, _ = parities()
    rounded = coeff_ref[...].astype(jnp.bfloat16).astype(jnp.float32)
    for k in range(kb):
        splat[k] = jnp.broadcast_to(rounded[:, k : k + 1], (8, BLK))

    @pl.loop(0, ny // 32)
    def _(i):
        rows = [pl.ds(pl.multiple_of(i * 32 + 16 * h, 16), 16) for h in range(2)]
        spots = [(z, part, slice(None)) for z in range(nz) for part in rows]
        acc = [iterate_ref[spot] for spot in spots]
        for k in range(kb):
            scale = jnp.concatenate([splat[k]] * 2, 0)
            for n, spot in enumerate(spots):
                acc[n] = acc[n] + scale * basis_ref[(k, *spot)].astype(jnp.float32)
        for n, spot in enumerate(spots):
            u_ref[spot] = acc[n]
        for n, part in enumerate(rows):
            us_ref[part] = jnp.where(core0, acc[len(rows) + n], acc[n])
            uc_ref[part] = jnp.where(core0, acc[n], acc[len(rows) + n])


def tiled(value):
    *lead, ny, nx = value.shape
    value = jnp.swapaxes(value.reshape(*lead, ny // 8, 8, nx // BLK, BLK), -3, -2)
    return value.reshape(*lead, ny * nx // BLK, BLK)


def untiled(value, nx):
    *lead, rows, _ = value.shape
    value = jnp.swapaxes(value.reshape(*lead, rows * BLK // (8 * nx), nx // BLK, 8, BLK), -3, -2)
    return value.reshape(*lead, rows * BLK // nx, nx)


def update(coeffs, iterate, basis):
    kb, nx = basis.shape[0], basis.shape[3]
    iterate, basis = tiled(iterate), tiled(basis)
    values = pl.pallas_call(
        update_kernel,
        out_shape=(f32(*iterate.shape), f32(*iterate.shape[1:]), f32(*iterate.shape[1:])),
        in_specs=[VMEM] * 3,
        out_specs=(VMEM,) * 3,
        scratch_shapes=[pltpu.VMEM((kb, 8, BLK), jnp.float32)],
        compiler_params=pltpu.CompilerParams(vmem_limit_bytes=16 << 20),
        cost_estimate=pl.CostEstimate(flops=1 << 24, bytes_accessed=2 * basis.size, transcendentals=0),
        name="update",
    )(coeffs.reshape(1, kb), iterate, basis)
    return [untiled(value, nx) for value in values]


def lane_gather(values, index):
    numbers = lax.GatherDimensionNumbers(
        offset_dims=(),
        collapsed_slice_dims=(1,),
        start_index_map=(1,),
        operand_batching_dims=(0,),
        start_indices_batching_dims=(0,),
    )
    return lax.gather(values, index[..., None], numbers, (1, 1), mode=lax.GatherScatterMode.PROMISE_IN_BOUNDS)


def sketch_kernel(
    u_ref, k_ref, rhs_ref, off_ref, flip_ref, same_ref, cross_ref, even_ref, odd_ref,
    out_ref, ue_ref, uo_ref, base_ref, wz_ref, wy_ref, part_ref,
    hz_ref, hy_ref, sem,
):
    nz, ny, nx = u_ref.shape
    core0, even = parities()
    has_cross, has_odd = inside()
    blocks = nx // BLK
    store = pltpu.make_async_copy(u_ref, out_ref, sem)
    store.start()

    for z in range(nz):
        low, high = u_ref[z, :1, :], u_ref[z, ny - 1 :, :]
        ue_ref[z : z + 1, :] = jnp.where(even, high, low)
        uo_ref[z : z + 1, :] = jnp.where(even, low, high)

    lane = lax.broadcasted_iota(jnp.int32, (8, BLK), 1)
    line = lax.broadcasted_iota(jnp.int32, (8, BLK), 0)
    odd_lines = odd_ref[...] * has_odd
    low_y = jnp.where(even, odd_lines, even_ref[...])
    high_y = jnp.where(even, even_ref[...], odd_lines)
    cells = [(z, q) for z in range(nz) for q in range(blocks)]

    def lanes(q):
        return slice(q * BLK, (q + 1) * BLK)

    def tile(ref, y):
        return {(z, q): ref[z, y : y + 8, lanes(q)] for z, q in cells}

    def up(tiles):
        return {c: pltpu.roll(t, 7, 0) for c, t in tiles.items()}

    u, k = tile(u_ref, 0), tile(k_ref, 0)
    u_up, k_up = up(u), up(k)
    below = None
    for y in range(0, ny, 8):
        rows = slice(y, y + 8)
        if y + 8 < ny:
            u_next, k_next = tile(u_ref, y + 8), tile(k_ref, y + 8)
            u_next_up, k_next_up = up(u_next), up(k_next)
        else:
            u_next = k_next = None
            u_next_up = {c: 0.0 for c in cells}
            k_next_up = {(z, q): high_y[z : z + 1, lanes(q)] for z, q in cells}
        between = {q: (k[0, q] + k[1, q]) * (u[0, q] - u[1, q]) for q in range(blocks)}
        above = {}
        for z in range(nz):
            swap = core0 if z else jnp.logical_not(core0)
            u_right = {q: pltpu.roll(u[z, q], BLK - 1, 1) for q in range(blocks)}
            k_right = {q: pltpu.roll(k[z, q], BLK - 1, 1) for q in range(blocks)}
            u_right[blocks] = k_right[blocks] = 0.0
            left = None
            for q in range(blocks):
                c = (z, q)
                pair = k[c] + jnp.where(swap, same_ref[rows, lanes(q)], cross_ref[rows, lanes(q)] * has_cross)
                wz = 0.5 * pair
                wz_ref[z, rows, lanes(q)] = wz
                hz_ref[z, rows, lanes(q)] = wz * u[c]
                total = pair * u[c]
                total = total - between[q] if z else total + between[q]
                flow = (k[c] + jnp.where(line == 7, k_next_up[c], k_up[c])) * (
                    u[c] - jnp.where(line == 7, u_next_up[c], u_up[c])
                )
                above[c] = pltpu.roll(flow, 1, 0)
                if y == 0:
                    edge = k[c] + low_y[z : z + 1, lanes(q)]
                    wy_ref[z : z + 1, lanes(q)] = 0.5 * edge[:1]
                    edge = edge * u[c]
                    hy_ref[z : z + 1, lanes(q)] = 0.5 * edge[:1]
                    before = -edge
                else:
                    before = below[c]
                if y == ny - 8:
                    edge = k[c] + high_y[z : z + 1, lanes(q)]
                    wy_ref[nz + z : nz + z + 1, lanes(q)] = 0.5 * edge[7:]
                    hy_ref[nz + z : nz + z + 1, lanes(q)] = 0.5 * (edge * u[c])[7:]
                total = total + (flow - jnp.where(line == 0, before, above[c]))
                flow = (k[c] + jnp.where(lane == BLK - 1, k_right[q + 1], k_right[q])) * (
                    u[c] - jnp.where(lane == BLK - 1, u_right[q + 1], u_right[q])
                )
                turned = pltpu.roll(flow, 1, 1)
                before = -k[c] * u[c] if q == 0 else left
                total = total + (flow - jnp.where(lane == 0, before, turned))
                left = turned
                base_ref[z, rows, lanes(q)] = (rhs_ref[z, rows, lanes(q)] - 0.05 * u[c]) - 0.5 * total
        below = above
        u, k, u_up, k_up = u_next, k_next, u_next_up, k_next_up

    sums = []
    block_of = jnp.right_shift(lax.broadcasted_iota(jnp.int32, (blocks, nx), 1), 7)
    widen = (block_of == lax.broadcasted_iota(jnp.int32, (blocks, nx), 0)).astype(jnp.float32).astype(jnp.bfloat16)

    def place(offs, signs):
        slot = lax.broadcasted_iota(jnp.int32, (ROWS, offs.shape[1]), 0)
        return jnp.where(slot == jnp.right_shift(offs, 7), signs, 0.0).astype(jnp.bfloat16)

    def turn(block, by):
        spot = lax.broadcasted_iota(jnp.int32, block.shape, 1)
        here = spot >= by
        block = lane_gather(block, (spot - by) & (BLK - 1))
        high = block.astype(jnp.bfloat16)
        low = (block - high.astype(jnp.float32)).astype(jnp.bfloat16)
        none = jnp.zeros_like(high)
        return [jnp.concatenate([jnp.where(here, t, none), jnp.where(here, none, t)], 1) for t in (high, low)]

    def add(spots, terms):
        at = jnp.concatenate(spots * 2, 1)
        values = jnp.concatenate([t[0] for t in terms] + [t[1] for t in terms], 0)
        sums.append(jnp.dot(at, values, preferred_element_type=jnp.float32))

    for z in range(nz):
        swap = core0 if z else jnp.logical_not(core0)
        theirs = jnp.where(swap, same_ref[ny:, : 2 * BLK], cross_ref[ny:, : 2 * BLK] * has_cross)
        mine = (2 * flip_ref[z] - 1).astype(jnp.float32)
        for source, offs, signs in (
            (base_ref, off_ref[z], mine),
            (hz_ref, theirs[:, :ny].astype(jnp.int32), theirs[:, BLK : BLK + ny]),
        ):
            turned = columns((offs & (BLK - 1)).astype(jnp.float32)).astype(jnp.bfloat16)
            turned = jnp.dot(turned, widen, preferred_element_type=jnp.float32).astype(jnp.int32)
            for start in range(0, blocks, GROUP):
                group = range(start, start + GROUP)
                at = place(
                    jnp.concatenate([offs[q : q + 1, :] for q in group], 1),
                    jnp.concatenate([signs[q : q + 1, :] for q in group], 1),
                )
                add([at], [turn(source[z, :, lanes(q)], turned[:, lanes(q)]) for q in group])

    hy_ref[2 * nz :, :] = jnp.zeros((16 - 2 * nz, nx), jnp.float32)
    unused = jnp.zeros((16 - 2 * nz, nx), jnp.float32)
    y_offs = jnp.concatenate([low_y[nz : 2 * nz], high_y[nz : 2 * nz], unused], 0).astype(jnp.int32)
    y_signs = jnp.concatenate([low_y[2 * nz : 3 * nz], high_y[2 * nz : 3 * nz], unused], 0)
    spots, terms = [], []
    for q in range(blocks):
        offs, signs = y_offs[:, lanes(q)], y_signs[:, lanes(q)]
        spots.append(place(jnp.transpose(offs[:, :1]), jnp.transpose(signs[:, :1])))
        terms.append(turn(hy_ref[:, lanes(q)], offs & (BLK - 1)))
    add(spots, terms)

    got = sum(sums[1:], sums[0])
    carry = got[:, BLK:]
    part = got[:, :BLK] + jnp.concatenate([carry[ROWS - 1 :], carry[: ROWS - 1]], 0)
    for m in range(ROWS):
        part_ref[m // blocks : m // blocks + 1, lanes(m % blocks)] = part[m : m + 1]
    store.wait()


def sketch(u, *rest):
    nz, ny, nx = u.shape
    field = f32(nz, ny, nx)
    return pl.pallas_call(
        sketch_kernel,
        out_shape=(
            field, f32(nz, nx), f32(nz, nx), field, field, f32(2 * nz, nx), f32(SK // nx, nx),
        ),
        in_specs=[VMEM] * 9,
        out_specs=(pl.BlockSpec(memory_space=pl.ANY),) + (VMEM,) * 6,
        scratch_shapes=[
            pltpu.VMEM((nz, ny, nx), jnp.float32),
            pltpu.VMEM((16, nx), jnp.float32),
            pltpu.SemaphoreType.DMA,
        ],
        compiler_params=pltpu.CompilerParams(vmem_limit_bytes=16 << 20),
        cost_estimate=pl.CostEstimate(flops=1 << 24, bytes_accessed=16 << 20, transcendentals=0),
        name="sketch",
    )(u, *rest)


def halo_kernel(base_ref, wz_ref, wy_ref, us_ref, uc_ref, ue_ref, uo_ref, res_ref):
    nz, ny, _ = base_ref.shape
    core0, even = parities()
    has_cross, has_odd = inside()
    odd_lines = uo_ref[...] * has_odd
    low_y = jnp.where(even, odd_lines, ue_ref[...])
    high_y = jnp.where(even, ue_ref[...], odd_lines)
    for z in range(nz):
        swap = core0 if z else jnp.logical_not(core0)
        for y in range(0, ny, 8):
            rows = slice(y, y + 8)
            value = base_ref[z, rows, :] + wz_ref[z, rows, :] * jnp.where(
                swap, us_ref[rows, :], uc_ref[rows, :] * has_cross
            )
            res_ref[z, rows, :] = value
        res_ref[z, :1, :] += wy_ref[z : z + 1, :] * low_y[z : z + 1, :]
        res_ref[z, ny - 1 :, :] += wy_ref[nz + z : nz + z + 1, :] * high_y[z : z + 1, :]


def with_halo(base, *rest):
    return pl.pallas_call(
        halo_kernel,
        out_shape=f32(*base.shape),
        in_specs=[VMEM] * 7,
        out_specs=VMEM,
        compiler_params=pltpu.CompilerParams(vmem_limit_bytes=8 << 20),
        cost_estimate=pl.CostEstimate(flops=1 << 20, bytes_accessed=2 << 20, transcendentals=0),
        name="halo",
    )(base, *rest)


def scale_kernel(*refs):
    sketch = refs[0][...]
    for ref in refs[1:-1]:
        sketch = sketch + ref[...]
    mean = jnp.sum(sketch * sketch) * (1.0 / SK)
    unit = sketch / jnp.sqrt(jnp.broadcast_to(mean + 1e-06, sketch.shape))
    wide = sketch.shape[1] // BLK
    for m in range(ROWS):
        refs[-1][m : m + 1, :] = unit[m // wide : m // wide + 1, m % wide * BLK : (m % wide + 1) * BLK]


def scaled(*parts):
    return pl.pallas_call(
        scale_kernel,
        out_shape=f32(ROWS, BLK),
        in_specs=[VMEM] * len(parts),
        out_specs=VMEM,
        compiler_params=pltpu.CompilerParams(vmem_limit_bytes=4 << 20),
        name="scaled",
    )(*parts)


def both_ways(pairs):
    return pairs + [(b, a) for a, b in pairs]


def pairs_from(first, count):
    return both_ways([(i, i + 1) for i in range(first, count - 1, 2)])


def rounds(count):
    pairs = {"pair": pairs_from(0, count)}
    if count == 2:
        return [pairs]
    if count == 4:
        return [{f"apart{k}": [(i, i ^ k) for i in range(4)] for k in (3, 2, 1)}]
    third = both_ways([(0, 5), (1, 4), (2, 7), (3, 6)])
    second = [(i, (i - 2) % 8) for i in range(0, 8, 2)] + [(i, (i + 2) % 8) for i in range(1, 8, 2)]
    first = both_ways([(i, (i + 1) % 8) for i in range(1, 8, 2)])
    return [pairs, {"apart3": third, "apart2": second, "apart1": first}]


def shards(sizes, *arrays):
    return cycle_end(sizes, *arrays)


def cycle_end(sizes, iterate, basis, coeffs, rhs, kappa, offsets, flips):
    gz = sizes["z"] * sizes["x"] * sizes["core"]
    gy = sizes["gy"]
    same, cross = pairs_from(0, gz), pairs_from(1, gz) + [(0, 0), (gz - 1, gz - 1)]
    even, odd = pairs_from(0, gy), pairs_from(1, gy) + [(0, 0), (gy - 1, gy - 1)]

    offsets, flips = jnp.swapaxes(offsets, 1, 2), jnp.swapaxes(flips, 1, 2)
    k_same, k_cross, k_even, k_odd = edges(kappa, offsets, flips)
    k_cross = lax.ppermute(k_cross, GZ, cross)
    k_same = lax.ppermute(k_same, GZ, same)
    k_even = lax.ppermute(k_even, "gy", even)
    k_odd = lax.ppermute(k_odd, "gy", odd)
    u, u_same, u_cross = update(coeffs, iterate, basis)
    u_out, u_even, u_odd, base, wz, wy, part = sketch(
        u, kappa, rhs, offsets, flips, k_same, k_cross, k_even, k_odd
    )
    u_same, part = lax.optimization_barrier((u_same, part))
    value = part + lax.ppermute(part, GZ, same)
    terms = [value]
    for axis in ("gy", "x", "z"):
        for step in rounds(sizes[axis]) if sizes[axis] > 1 else ():
            value = sum(terms[1:], terms[0])
            if axis == "x":
                u_cross, value = lax.optimization_barrier((u_cross, value))
            terms = [value] + [lax.ppermute(value, axis, pairs) for pairs in step.values()]
    u_cross = lax.ppermute(u_cross, GZ, cross)
    u_same = lax.ppermute(u_same, GZ, same)
    u_even = lax.ppermute(u_even, "gy", even)
    u_odd = lax.ppermute(u_odd, "gy", odd)
    residual = with_halo(base, wz, wy, u_same, u_cross, u_even, u_odd)
    return u_out, residual, scaled(*terms).reshape(SK)


def build(mesh, outer):
    gy = mesh.shape["gy"]
    finer = Mesh(mesh.devices.reshape(*outer, gy), (*GZ, "gy"))
    sizes = dict(finer.shape)
    field = P(GZ, "gy", None)
    return jax.shard_map(
        functools.partial(shards, sizes),
        mesh=finer,
        in_specs=(field, P(None, GZ, "gy", None), P(), field, field, field, field),
        out_specs=(field, field, P()),
        check_vma=False,
    )


def solution(mesh):
    return build(mesh, (mesh.shape["gz"] // 8, 4, 2))
```
